128 devices in a mesh: trial: 32 (over z, y, core), geno: 4 (over x).
Axes of the slice: x: 4, y: 4, z: 4, core: 2. Of those that a mesh axis runs over, the one named last changes fastest.
Arguments:
- probe_signs: int32 [16, 128, 1, 44, 256], P(None, ('trial', 'geno')), may hold values 0 or 1
- trial_rows: int32 [32], P('trial'), may hold values from 89 to 176
- trial_cols: int32 [32], P('trial'), may hold values from 128 to 256
- ar_rho: float32 [32, 2], P('trial'), may hold values from 0.1 to 0.7
- res_var: float32 [32], P('trial'), may hold values from 4 to 16
- plot_owner: int32 [128, 1, 44, 256, 1], P(('trial', 'geno')), may hold values from 0 to 127; in each aligned block of 11264 rows (0 to 11263, 11264 to 22527, ..., all dimensions but the last counted through in order) at most 176 rows name the same one
- plot_slot: int32 [128, 1, 44, 256], P(('trial', 'geno')), may hold values from 0 to 1023
Outputs:
- geno_terms: float32 [3, 16, 131072], P(None, None, ('trial', 'geno'))
The draws below stay inside these ranges and needn't reach their ends.
Inputs may be any that keep to these rules, and one draw needn't show every extreme that they name: `plot_owner`: among the plot positions of one device at most 176 name the same owner, and in every draw some device has exactly 176 positions for one owner. A plot's genotype is 1024 * plot_owner + plot_slot.
All inputs are finite; a program needn't handle non-finite values. No bound on the sum of `probe_signs` on one device may be relied on, other than what follows from the above.
Results may differ from the reference program's by a relative error of at most 0.0028.
Values may be sent and summed in bfloat16 or wider, within the bound.
A program may use at most 64 MiB of HBM per device.

```python
import math
import jax
import jax.numpy as jnp
import numpy as np

PROBES = 16
FR = 44
FC = 256
TILES_DEV = 1
G_DEV = 1024
FIELD_ROWS = 176
TRIALS = 32
P_DEV = 11264
CAP = 176
G = 131072
N_TRIAL = 32
N_GENO = 4
DEVICES = 128


def set_ends(entries, rng, smallest, top_value):
    extent = entries.shape
    index_at = [jax.random.randint(jax.random.fold_in(rng, axis), (), 0, extent[axis]) for axis in range(len(extent))]
    entries = entries.at[tuple(index_at)].set(smallest)
    longest = extent.index(max(extent))
    index_at[longest] = (index_at[longest] + 1) % extent[longest]
    return entries.at[tuple(index_at)].set(top_value)


def steps_of(key, extent, cuts, least, largest):
    def one(position, parts):
        draws = jax.random.uniform(jax.random.fold_in(jax.random.fold_in(key, 6), position), (parts,), jnp.float32, least / len(cuts), largest / len(cuts))
        return jnp.repeat(jnp.exp(draws), extent[position] // parts).reshape((-1,) + (1,) * (len(extent) - position - 1))

    loudness = one(*cuts[0])
    for cut in cuts[1:]:
        loudness = loudness * one(*cut)
    return loudness


def shared_out(rng, own, number, rows, count, top, most, skew):
    order = jax.random.permutation(rng, count)
    packed, common = portions_of(count, rows * top, most, skew, True), portions_of(count, rows * top, most, skew, False)
    places = jnp.arange(count)

    def named(sizes, rotation):
        used = int((sizes > 0).sum())
        fixed = max(1, used // 4)
        moved = fixed + (places - fixed + rotation * (used - fixed)) % max(1, count - fixed)
        return jnp.zeros((count,), jnp.int32).at[order[jnp.where(places < fixed, places, moved)]].set(jnp.asarray(sizes, jnp.int32))

    sizes = jnp.where(number % 4 == 0, named(packed, number // 4), named(common, number - number // 4 - 1))
    mixed = jax.random.permutation(jax.random.fold_in(own, 3), count)
    giver, taker = mixed[0:count // 2 * 2:2], mixed[1:count // 2 * 2:2]
    margin = jnp.minimum(sizes[giver] - 1, most - sizes[taker]) // 2
    margin = jnp.where((giver == order[0]) | (taker == order[0]) | (sizes[taker] == 0), 0, jnp.maximum(margin, 0))
    moved = jax.random.randint(jax.random.fold_in(own, 4), (count // 2,), 0, 1 << 20) % (margin + 1)
    sizes = sizes.at[giver].add(-moved).at[taker].add(moved)
    members = jnp.searchsorted(jnp.cumsum(sizes), jnp.arange(rows * top), side="right").astype(jnp.int32)
    table = members.reshape(top, rows).T
    table = table[jax.random.permutation(jax.random.fold_in(own, 1), rows)]
    rotation = jax.random.randint(jax.random.fold_in(own, 2), (rows, 1), 0, top)
    return jnp.take_along_axis(table, (jnp.arange(top)[None, :] + rotation) % top, axis=1)


def portions_of(number_of, total, bound, skew, full):
    loads = [(1 << 20) // math.isqrt(grade ** skew) + 1 for grade in range(1, number_of + 1)]
    largest = bound if full else min(bound, max(-(-total // number_of), total * loads[0] // sum(loads)))
    least = 1 if total - largest >= number_of - 1 else 0
    holding, spare = [largest] + [least] * (number_of - 1), total - largest - least * (number_of - 1)
    while spare > 0:
        movable = [i for i in range(1, number_of) if holding[i] < largest] or [i for i in range(1, number_of) if holding[i] < bound]
        pool, remaining = sum([loads[i] for i in movable]), spare
        for i in movable:
            addition = min(bound - holding[i], max(1, remaining * loads[i] // pool), spare)
            holding[i] = holding[i] + addition
            spare = spare - addition
    return np.array(holding)


def setup_inputs(seed: int = 0) -> dict:
    keys = jax.random.split(jax.random.key(seed), 8)
    probe_signs = set_ends((jax.random.randint(keys[0], (PROBES, DEVICES, TILES_DEV, FR, FC), 0, 2) < 1).astype(jnp.int32), jax.random.fold_in(keys[0], 1), 0, 1)
    trial_rows = set_ends(jax.random.randint(keys[1], (TRIALS,), 2 * FR + 1, FIELD_ROWS + 1), jax.random.fold_in(keys[1], 1), 2 * FR + 1, FIELD_ROWS).astype(jnp.int32)
    trial_cols = set_ends(jax.random.randint(keys[2], (TRIALS,), FC // 2, FC + 1), jax.random.fold_in(keys[2], 1), FC // 2, FC).astype(jnp.int32)
    ar_rho = jnp.clip(0.1 + 0.59999999 * jax.random.uniform(keys[3], (TRIALS, 2), jnp.float32) ** steps_of(keys[3], (TRIALS, 2), ((0, 32),), -0.2, 0.2), 0.1, 0.7)
    res_var = jnp.clip(jnp.exp(math.log(16.0) - 1.3862944 * jax.random.uniform(keys[4], (TRIALS,), jnp.float32) ** steps_of(keys[4], (TRIALS,), ((0, 32),), -0.2, 0.2)), 4.0, 16.0)
    plot_owner_keys = jax.random.split(jax.random.fold_in(keys[5], 1), DEVICES * TILES_DEV * FR * FC // P_DEV)
    plot_owner_turns = jax.random.permutation(jax.random.fold_in(keys[5], 3), DEVICES * TILES_DEV * FR * FC // P_DEV)
    plot_owner = jax.vmap(lambda own, number: shared_out(jax.random.fold_in(keys[5], 2), own, number, P_DEV, DEVICES, 1, CAP, 2))(plot_owner_keys, plot_owner_turns).reshape((DEVICES, TILES_DEV, FR, FC, 1))
    plot_slot = set_ends(jax.random.randint(keys[6], (DEVICES, TILES_DEV, FR, FC), 0, G_DEV), jax.random.fold_in(keys[6], 1), 0, G_DEV - 1).astype(jnp.int32)
    return {"probe_signs": probe_signs, "trial_rows": trial_rows, "trial_cols": trial_cols, "ar_rho": ar_rho, "res_var": res_var, "plot_owner": plot_owner, "plot_slot": plot_slot}


def line_coeffs(rho_vals, cell_count, positions):
    inverse = 1.0 / (1.0 - rho_vals * rho_vals)
    edge_mask = (positions[None, :] == 0) | (positions[None, :] == cell_count[:, None] - 1)
    inside = 1.0 + rho_vals * rho_vals
    main_diag = jnp.where(edge_mask, inverse[:, None], (inverse * inside)[:, None])
    main_slope = jnp.where(edge_mask, (2.0 * rho_vals * inverse * inverse)[:, None], (4.0 * rho_vals * inverse * inverse)[:, None])
    off_diag = -inverse * rho_vals
    off_slope = -inside * inverse * inverse
    return main_diag, off_diag, main_slope, off_slope


def across_columns(field_vals, main_diag, off_diag):
    padded = jnp.pad(field_vals, ((0, 0), (0, 0), (0, 0), (1, 1)))
    return main_diag[:, None, :] * field_vals + off_diag[:, None, None] * (padded[..., :-2] + padded[..., 2:])


def across_rows(padded, main_diag, off_diag):
    return main_diag[:, :, None] * padded[:, :, 1:-1, :] + off_diag[:, None, None] * (padded[:, :, :-2, :] + padded[:, :, 2:, :])


def reference(probe_signs, trial_rows, trial_cols, ar_rho, res_var, plot_owner, plot_slot):
    probe_count = probe_signs.shape[0]
    stacked = probe_signs.reshape(probe_count, N_TRIAL, N_GENO, TILES_DEV, FR, FC)
    stacked = stacked.transpose(0, 1, 3, 2, 4, 5).reshape(probe_count, TRIALS, FIELD_ROWS, FC)
    row_pos = jnp.arange(FIELD_ROWS, dtype=jnp.int32)
    col_pos = jnp.arange(FC, dtype=jnp.int32)
    present = (row_pos[None, :, None] < trial_rows[:, None, None]) & (col_pos[None, None, :] < trial_cols[:, None, None])
    probe_field = jnp.where(present[None], 2.0 * stacked.astype(jnp.float32) - 1.0, jnp.float32(0.0))
    col_diag, col_off, col_sdiag, col_soff = line_coeffs(ar_rho[:, 1], trial_cols, col_pos)
    row_diag, row_off, row_sdiag, row_soff = line_coeffs(ar_rho[:, 0], trial_rows, row_pos)
    col_field = across_columns(probe_field, col_diag, col_off)
    col_slope = across_columns(probe_field, col_sdiag, col_soff)
    plot_scale = jnp.where(present, (1.0 / res_var)[:, None, None], jnp.float32(0.0))
    pad_rows = ((0, 0), (0, 0), (1, 1), (0, 0))
    field_pad = jnp.pad(col_field, pad_rows)
    slope_pad = jnp.pad(col_slope, pad_rows)
    genotype = (plot_owner.reshape(-1) * G_DEV + plot_slot.reshape(-1)).astype(jnp.int32)
    results = []
    for image in (across_rows(field_pad, row_diag, row_off), across_rows(field_pad, row_sdiag, row_soff), across_rows(slope_pad, row_diag, row_off)):
        plot_terms = (image * plot_scale[None]).astype(jnp.bfloat16)
        flat_terms = plot_terms.reshape(probe_count, N_TRIAL, TILES_DEV, N_GENO, FR, FC)
        flat_terms = flat_terms.transpose(0, 1, 3, 2, 4, 5).reshape(probe_count, -1).astype(jnp.float32)
        summed = jax.ops.segment_sum(flat_terms.T, genotype, num_segments=G)
        results.append(summed.T)
    return jnp.stack(results, 0)
```

```python
import functools

import jax
import jax.numpy as jnp
from jax import lax
from jax.experimental import pallas as pl
from jax.experimental.pallas import tpu as pltpu
from jax.sharding import PartitionSpec as P

G_DEV = 1024
PROBES = 16
FR = 44
FC = 256
DEVICES = 128
PER_ROW = 5
WORDS = 24
SLOTS = 176
ROWS = 36
PAD_ROWS = 40
BATCH = 16
BATCHES = DEVICES // BATCH
STEP = 37
SCALE_BITS = 24
MESH = pl.DeviceIdType.MESH
F32 = jnp.float32
BF16 = jnp.bfloat16
I32 = jnp.int32


def shifted(k):
    trial, geno = lax.axis_index("trial"), lax.axis_index("geno")
    core = lax.rem(lax.rem(trial, 2) + k // 64, 2)
    y = lax.rem(lax.rem(trial // 2, 4) + lax.rem(k // 4, 4), 4)
    z = lax.rem(trial // 8 + lax.rem(k // 16, 4), 4)
    x = lax.rem(geno + lax.rem(k, 4), 4)
    return z * 8 + y * 2 + core, x


def kernel(
    signs_ref, rows_ref, cols_ref, rho_ref, var_ref, owner_ref, slot_ref, out_ref,
    xs, us, vs, halo, table, picks, picks_s, sbuf, rbuf, digits, acc,
    in_sem, pick_sem, halo_send, halo_recv, send_sem, recv_sem,
):
    trial, geno = lax.axis_index("trial"), lax.axis_index("geno")
    barrier = pltpu.get_barrier_semaphore()

    loads = [
        pltpu.make_async_copy(signs_ref.at[p], xs.at[:, p, :], in_sem.at[p]) for p in range(PROBES)
    ]
    for load in loads:
        load.start()

    def greet(k, carry):
        pl.semaphore_signal(barrier, inc=1, device_id=shifted(k), device_id_type=MESH)
        return carry

    lax.fori_loop(1, DEVICES, greet, 0)

    owner_id = lax.broadcasted_iota(I32, (DEVICES, FC), 0)
    col_i = lax.broadcasted_iota(I32, (FC, FC), 0)
    col_j = lax.broadcasted_iota(I32, (FC, FC), 1)
    upto = jnp.where(col_i <= col_j, F32(1), F32(0)).astype(BF16)
    place_id = lax.broadcasted_iota(I32, (SLOTS, FC), 0)
    col_f = lax.broadcasted_iota(I32, (1, FC), 1).astype(F32)
    digits[...] = jnp.zeros_like(digits)

    def rank_row(r, running):
        own = owner_id == owner_ref[pl.ds(r, 1), :]
        hot = jnp.where(own, F32(1), F32(0)).astype(BF16)
        count = jnp.dot(hot, upto, preferred_element_type=F32) + running
        place = jnp.sum(jnp.where(own, count, F32(0)), axis=0, keepdims=True) - 1.0
        at_place = place_id == place.astype(I32)
        row_no = (r + 1).astype(F32)
        carry_row = jnp.where(at_place, row_no, F32(0))
        carry_col = jnp.where(at_place, col_f, F32(0))
        both = jnp.concatenate([carry_row, carry_col], axis=0).astype(BF16)
        digits[...] += lax.dot_general(
            hot, both, (((1,), (1,)), ((), ())), preferred_element_type=F32
        )
        return jnp.broadcast_to(count[:, FC - 1 :], (DEVICES, FC))

    def rank_rows(q, running):
        for i in range(4):
            running = rank_row(q * 4 + i, running)
        return running

    lax.fori_loop(0, FR // 4, rank_rows, jnp.zeros((DEVICES, FC), F32))
    chosen = (digits[:, :SLOTS] * float(FC) + digits[:, SLOTS:]).astype(I32)
    picks[:, :SLOTS] = jnp.clip(chosen, 0, (FR + 1) * FC - 1)
    picks[:, SLOTS:] = jnp.zeros((DEVICES, FC - SLOTS), I32)
    to_smem = pltpu.make_async_copy(picks, picks_s, pick_sem)
    to_smem.start()

    n_rows, n_cols = rows_ref[0], cols_ref[0]
    rho_r = jnp.full((1, FC), rho_ref[0, 0], F32)
    rho_c = jnp.full((1, FC), rho_ref[0, 1], F32)
    res = jnp.full((1, FC), var_ref[0], F32)
    col = lax.broadcasted_iota(I32, (1, FC), 1)

    def line(rho):
        inv = 1.0 / (1.0 - rho * rho)
        inside = 1.0 + rho * rho
        return (
            (inv, inv * inside, -inv * rho),
            (2.0 * rho * inv * inv, 4.0 * rho * inv * inv, -inside * inv * inv),
        )

    (ce, ci, co), (cse, csi, cso) = line(rho_c)
    (re, ri, ro), (rse, rsi, rso) = line(rho_r)
    col_edge = (col == 0) | (col == n_cols - 1)
    cd = jnp.where(col_edge, ce, ci)
    csd = jnp.where(col_edge, cse, csi)
    in_col = col < n_cols
    left_ok = col > 0
    right_ok = col < FC - 1
    inv_res = 1.0 / res
    c_top = jnp.maximum(ce, ci) - 2.0 * co
    cs_top = jnp.maximum(cse, csi) - 2.0 * cso
    r_top = jnp.maximum(re, ri) - 2.0 * ro
    rs_top = jnp.maximum(rse, rsi) - 2.0 * rso
    tops = [r_top * c_top * inv_res, rs_top * c_top * inv_res, r_top * cs_top * inv_res]
    scale_ints = [jnp.ceil(top * float(1 << SCALE_BITS)).astype(I32) + 1 for top in tops]
    gains = [
        inv_res * 32766.0 / (s.astype(F32) * (1.0 / float(1 << SCALE_BITS))) for s in scale_ints
    ]
    sub8 = lax.broadcasted_iota(I32, (8, FC), 0)
    scale_rows = jnp.where(
        sub8 == 5, scale_ints[0], jnp.where(sub8 == 6, scale_ints[1], scale_ints[2])
    )

    lane = lax.broadcasted_iota(I32, (1, 128), 1)
    group = jnp.where(lane < PER_ROW * WORDS, lane // WORDS, lane - PER_ROW * WORDS)
    group = jnp.where(group >= PER_ROW, 0, group)
    masks = [group == j for j in range(PER_ROW)]
    lane8 = lax.broadcasted_iota(I32, (8, 128), 1)
    first_scales = jnp.where(
        lane8 == 125, scale_ints[0][:, :128],
        jnp.where(lane8 == 126, scale_ints[1][:, :128], scale_ints[2][:, :128]),
    )
    table[0:8, :] = jnp.where(lane8 >= 125, first_scales, jnp.where(lane8 >= 120, -1, 0))

    for load in loads:
        load.wait()

    def columns(bits, row):
        present = in_col & (row >= 0) & (row < n_rows)
        p = jnp.where(present, 2.0 * bits.astype(F32) - 1.0, F32(0))
        beside = jnp.where(left_ok, pltpu.roll(p, 1, 1), F32(0)) + jnp.where(
            right_ok, pltpu.roll(p, FC - 1, 1), F32(0)
        )
        return cd * p + co * beside, csd * p + cso * beside

    def columns_row(r, carry):
        u, v = columns(xs[r], geno * FR + r)
        us[r + 1] = u
        vs[r + 1] = v
        return carry

    lax.fori_loop(0, FR, columns_row, 0)

    def terms_row(r, carry):
        row = geno * FR + r
        edge = (row == 0) | (row == n_rows - 1)
        rd = jnp.where(edge, re, ri)
        rsd = jnp.where(edge, rse, rsi)
        present = in_col & (row < n_rows)
        k0, k1, k2 = [jnp.where(present, gain, F32(0)) for gain in gains]
        u, v = us[r + 1], vs[r + 1]
        u2 = us[r] + us[r + 2]
        v2 = vs[r] + vs[r + 2]
        values = [
            (rd * u + ro * u2) * k0,
            (rsd * u + rso * u2) * k1,
            (rd * v + ro * v2) * k2,
        ]
        words = []
        for value in values:
            q = jnp.floor(value + 0.5).astype(I32)
            words.append((q[8:] << 16) | (q[:8] & 0xFFFF))
        aux = jnp.where(sub8 < PER_ROW, slot_ref[pl.ds(r, 1), :], scale_rows)
        stacked = jnp.concatenate(words * PER_ROW + [aux], axis=0)
        table[pl.ds(pl.multiple_of((r + 1) * FC, FC), FC), :] = stacked.T
        return carry

    lax.fori_loop(1, FR - 1, terms_row, 0)

    pl.semaphore_wait(barrier, DEVICES - 1)
    above = (trial, lax.rem(geno + 3, 4))
    below = (trial, lax.rem(geno + 1, 4))
    edges = [
        pltpu.make_async_remote_copy(
            src_ref=xs.at[0], dst_ref=halo.at[1], send_sem=halo_send.at[0],
            recv_sem=halo_recv.at[1], device_id=above, device_id_type=MESH,
        ),
        pltpu.make_async_remote_copy(
            src_ref=xs.at[FR - 1], dst_ref=halo.at[0], send_sem=halo_send.at[1],
            recv_sem=halo_recv.at[0], device_id=below, device_id_type=MESH,
        ),
    ]
    for edge in edges:
        edge.start()
    for edge in edges:
        edge.wait()
    for side, r in ((0, -1), (1, FR)):
        row = jnp.where((geno == 0) & (side == 0), -1, geno * FR + r)
        u, v = columns(halo[side], row)
        us[r + 1] = u
        vs[r + 1] = v
    lax.fori_loop(0, 2, lambda i, carry: terms_row(i * (FR - 1), carry), 0)
    to_smem.wait()

    def gather(target, dst):
        for r in range(ROWS):
            row = None
            for j in range(PER_ROW):
                slot = min(r * PER_ROW + j, FC - 1)
                part = table[pl.ds(picks_s[target, slot], 1), :]
                row = part if row is None else jnp.where(masks[j], part, row)
            dst[pl.ds(r, 1), :] = row

    def copy_of(s):
        k = lax.rem(s * STEP, DEVICES)
        t, g = shifted(k)
        return pltpu.make_async_remote_copy(
            src_ref=sbuf.at[s], dst_ref=rbuf.at[s, pl.ds(0, ROWS)],
            send_sem=send_sem.at[s], recv_sem=recv_sem.at[s],
            device_id=(t, g), device_id_type=MESH,
        )

    gather(trial * 4 + geno, rbuf.at[0])
    acc[...] = jnp.zeros_like(acc)

    def fill(s, carry):
        t, g = shifted(lax.rem(s * STEP, DEVICES))
        gather(t * 4 + g, sbuf.at[s])

        @pl.when(s > 1)
        def _():
            copy_of(s - 1).start()

        return carry

    width = BATCH * PAD_ROWS
    high_id = lax.broadcasted_iota(I32, (FC, width), 0)
    pos = lax.rem(lax.broadcasted_iota(I32, (1, width), 1), PAD_ROWS)

    def add_batch(b):
        def arrive(s, carry):
            copy_of(s).wait_recv()
            return carry

        lax.fori_loop(jnp.maximum(b * BATCH, 1), (b + 1) * BATCH, arrive, 0)
        block = rbuf[pl.ds(b * BATCH, BATCH)].reshape(width, 128).T
        scales = [
            block[125 + t : 126 + t, :].astype(F32) * (1.0 / (float(1 << SCALE_BITS) * 32766.0))
            for t in range(3)
        ]
        total = acc[...]
        for j in range(PER_ROW):
            slot = jnp.where(pos < ROWS, block[120 + j : 121 + j, :], -1)
            low = slot >> 8
            hot = jnp.where(high_id == (slot & 255), F32(1), F32(0)).astype(BF16)
            parts = []
            for t in range(3):
                word = block[(j * 3 + t) * 8 : (j * 3 + t + 1) * 8, :]
                parts.append(((word << 16) >> 16).astype(F32) * scales[t])
                parts.append((word >> 16).astype(F32) * scales[t])
            values = jnp.concatenate(parts, axis=0)
            split = jnp.concatenate(
                [jnp.where(low == q, values, F32(0)) for q in range(4)], axis=0
            ).astype(BF16)
            total = total + lax.dot_general(
                split, hot, (((1,), (1,)), ((), ())), preferred_element_type=F32
            )
        acc[...] = total

    def stage(b, carry):
        lax.fori_loop(jnp.maximum(b * BATCH, 1), (b + 1) * BATCH, fill, 0)

        @pl.when(b >= 2)
        def _():
            add_batch(b - 2)

        return carry

    lax.fori_loop(0, BATCHES, stage, 0)
    copy_of(DEVICES - 1).start()
    add_batch(BATCHES - 2)
    add_batch(BATCHES - 1)
    for q in range(4):
        out_ref[:, q * FC : (q + 1) * FC] = acc[q * 48 : (q + 1) * 48, :]

    def sent(s, carry):
        copy_of(s).wait_send()
        return carry

    lax.fori_loop(1, DEVICES, sent, 0)


def body(probe_signs, trial_rows, trial_cols, ar_rho, res_var, plot_owner, plot_slot):
    smem = pl.BlockSpec(memory_space=pltpu.SMEM)
    vmem = pl.BlockSpec(memory_space=pltpu.VMEM)
    out = pl.pallas_call(
        kernel,
        out_shape=jax.ShapeDtypeStruct((3 * PROBES, G_DEV), F32),
        in_specs=[pl.BlockSpec(memory_space=pl.ANY), smem, smem, smem, smem, vmem, vmem],
        out_specs=vmem,
        scratch_shapes=[
            pltpu.VMEM((FR, PROBES, FC), I32),
            pltpu.VMEM((FR + 2, PROBES, FC), F32),
            pltpu.VMEM((FR + 2, PROBES, FC), F32),
            pltpu.VMEM((2, PROBES, FC), I32),
            pltpu.VMEM(((FR + 1) * FC, 128), I32),
            pltpu.VMEM((DEVICES, FC), I32),
            pltpu.SMEM((DEVICES, FC), I32),
            pltpu.VMEM((DEVICES, ROWS, 128), I32),
            pltpu.VMEM((DEVICES, PAD_ROWS, 128), I32),
            pltpu.VMEM((DEVICES, 2 * SLOTS), F32),
            pltpu.VMEM((12 * PROBES, FC), F32),
            pltpu.SemaphoreType.DMA((PROBES,)),
            pltpu.SemaphoreType.DMA,
            pltpu.SemaphoreType.DMA((2,)),
            pltpu.SemaphoreType.DMA((2,)),
            pltpu.SemaphoreType.DMA((DEVICES,)),
            pltpu.SemaphoreType.DMA((DEVICES,)),
        ],
        compiler_params=pltpu.CompilerParams(
            collective_id=0, has_side_effects=True, vmem_limit_bytes=56 << 20
        ),
        name="hutchinson_exchange",
    )(
        probe_signs.reshape(PROBES, FR, FC),
        trial_rows,
        trial_cols,
        ar_rho,
        res_var,
        plot_owner.reshape(FR, FC),
        plot_slot.reshape(FR, FC),
    )
    return out.reshape(3, PROBES, G_DEV)


def solution(mesh):
    return jax.shard_map(
        body,
        mesh=mesh,
        in_specs=(
            P(None, ("trial", "geno"), None, None, None),
            P("trial"),
            P("trial"),
            P("trial", None),
            P("trial"),
            P(("trial", "geno"), None, None, None, None),
            P(("trial", "geno"), None, None, None),
        ),
        out_specs=P(None, None, ("trial", "geno")),
        check_vma=False,
    )
```

```python
import jax
import jax.numpy as jnp
from jax import lax
from jax.experimental import pallas as pl
from jax.experimental.pallas import tpu as pltpu
from jax.sharding import PartitionSpec as P

G_DEV = 1024
PROBES = 16
FR = 44
FC = 256
DEVICES = 128
PER_ROW = 5
WORDS = 24
SLOTS = 176
ROWS = 36
PAD_ROWS = 40
BATCH = 16
BATCHES = DEVICES // BATCH
RANK_ROWS = 4
TERM_ROWS = 3
SCALE_BITS = 24
MESH = pl.DeviceIdType.MESH
F32 = jnp.float32
BF16 = jnp.bfloat16
I32 = jnp.int32


def places():
    trial, geno = lax.axis_index("trial"), lax.axis_index("geno")
    return trial // 8, lax.rem(trial // 2, 4), lax.rem(trial, 2), geno


def shifted(step, i):
    z, y, core, x = places()
    far = step // 4
    near = lax.rem(step, 4)
    tz = lax.rem(z + lax.rem(far, 4) + 2 * near + i, 4)
    ty = lax.rem(y + near, 4)
    tc = lax.rem(core + far // 4 + near + i // 2, 2)
    return tz * 8 + ty * 2 + tc, lax.rem(x + i, 4)


def kernel(
    signs_ref, rows_ref, cols_ref, rho_ref, var_ref, owner_ref, slot_ref, out_ref,
    xs, us, vs, halo, table, picks, picks_s, sbuf, rbuf, digits, acc,
    in_sem, pick_sem, halo_send, halo_recv, send_sem, recv_sem,
):
    trial, geno = lax.axis_index("trial"), lax.axis_index("geno")
    barrier = pltpu.get_barrier_semaphore()

    loads = [
        pltpu.make_async_copy(signs_ref.at[p, :, 0], xs.at[:, p, :], in_sem.at[p])
        for p in range(PROBES)
    ]
    for load in loads:
        load.start()

    def signal(step, i):
        pl.semaphore_signal(barrier, inc=1, device_id=shifted(step, i), device_id_type=MESH)

    def greet(step, carry):
        for i in range(4):
            signal(step, i)
        return carry

    for i in range(1, 4):
        signal(0, i)
    lax.fori_loop(1, DEVICES // 4, greet, 0)

    owner_id = lax.broadcasted_iota(I32, (DEVICES, FC), 0)
    col_i = lax.broadcasted_iota(I32, (FC, FC), 0)
    col_j = lax.broadcasted_iota(I32, (FC, FC), 1)
    upto = jnp.where(col_i <= col_j, F32(1), F32(0)).astype(BF16)
    place_id = lax.broadcasted_iota(I32, (SLOTS, FC), 0)
    col_f = lax.broadcasted_iota(I32, (1, FC), 1).astype(F32)
    digits[...] = jnp.zeros_like(digits)

    def rank_rows(q, running):
        lefts, rights = [], []
        for i in range(RANK_ROWS):
            r = q * RANK_ROWS + i
            own = owner_id == owner_ref[r]
            hot = jnp.where(own, F32(1), F32(0)).astype(BF16)
            count = jnp.dot(hot, upto, preferred_element_type=F32) + running
            running = jnp.broadcast_to(count[:, FC - 1 :], (DEVICES, FC))
            place = jnp.sum(jnp.where(own, count, F32(0)), axis=0, keepdims=True) - 1.0
            lefts.append(jnp.where(place_id == place.astype(I32), F32(1), F32(0)).astype(BF16))
            row_no = (r + 1).astype(F32)
            rights.append(
                jnp.concatenate(
                    [jnp.where(own, row_no, F32(0)), jnp.where(own, col_f, F32(0))], axis=0
                ).astype(BF16)
            )
        digits[...] += lax.dot_general(
            jnp.concatenate(lefts, axis=1), jnp.concatenate(rights, axis=1),
            (((1,), (1,)), ((), ())), preferred_element_type=F32,
        )
        return running

    lax.fori_loop(0, FR // RANK_ROWS, rank_rows, jnp.zeros((DEVICES, FC), F32))
    plot = (digits[:, :DEVICES] * float(FC) + digits[:, DEVICES:]).astype(I32)
    picks[...] = jnp.clip(plot, 0, (FR + 1) * FC - 1)
    to_smem = pltpu.make_async_copy(picks, picks_s, pick_sem)
    to_smem.start()

    n_rows, n_cols = rows_ref[0], cols_ref[0]
    rho_r = jnp.full((1, FC), rho_ref[0, 0], F32)
    rho_c = jnp.full((1, FC), rho_ref[0, 1], F32)
    res = jnp.full((1, FC), var_ref[0], F32)
    col = lax.broadcasted_iota(I32, (1, FC), 1)

    def line(rho):
        inv = 1.0 / (1.0 - rho * rho)
        inside = 1.0 + rho * rho
        return (
            (inv, inv * inside, -inv * rho),
            (2.0 * rho * inv * inv, 4.0 * rho * inv * inv, -inside * inv * inv),
        )

    (ce, ci, co), (cse, csi, cso) = line(rho_c)
    (re, ri, ro), (rse, rsi, rso) = line(rho_r)
    col_edge = (col == 0) | (col == n_cols - 1)
    cd = jnp.where(col_edge, ce, ci)
    csd = jnp.where(col_edge, cse, csi)
    in_col = col < n_cols
    left_ok = col > 0
    right_ok = col < FC - 1
    inv_res = 1.0 / res
    c_top = jnp.maximum(ce, ci) - 2.0 * co
    cs_top = jnp.maximum(cse, csi) - 2.0 * cso
    r_top = jnp.maximum(re, ri) - 2.0 * ro
    rs_top = jnp.maximum(rse, rsi) - 2.0 * rso
    tops = [r_top * c_top * inv_res, rs_top * c_top * inv_res, r_top * cs_top * inv_res]
    scale_ints = [jnp.ceil(top * float(1 << SCALE_BITS)).astype(I32) + 1 for top in tops]
    gains = [
        inv_res * 32766.0 / (s.astype(F32) * (1.0 / float(1 << SCALE_BITS))) for s in scale_ints
    ]
    sub8 = lax.broadcasted_iota(I32, (8, FC), 0)
    scale_rows = jnp.where(
        sub8 == 5, scale_ints[0], jnp.where(sub8 == 6, scale_ints[1], scale_ints[2])
    )

    lane = lax.broadcasted_iota(I32, (1, 128), 1)
    group = jnp.where(lane < PER_ROW * WORDS, lane // WORDS, lane - PER_ROW * WORDS)
    group = jnp.where(group >= PER_ROW, 0, group)
    masks = [group == j for j in range(PER_ROW)]
    lane8 = lax.broadcasted_iota(I32, (8, 128), 1)
    first_scales = jnp.where(
        lane8 == 125, scale_ints[0][:, :128],
        jnp.where(lane8 == 126, scale_ints[1][:, :128], scale_ints[2][:, :128]),
    )
    table[0:8, :] = jnp.where(lane8 >= 125, first_scales, jnp.where(lane8 >= 120, -1, 0))

    for load in loads:
        load.wait()

    def columns(bits, row):
        present = in_col & (row >= 0) & (row < n_rows)
        p = jnp.where(present, 2.0 * bits.astype(F32) - 1.0, F32(0))
        beside = jnp.where(left_ok, pltpu.roll(p, 1, 1), F32(0)) + jnp.where(
            right_ok, pltpu.roll(p, FC - 1, 1), F32(0)
        )
        return cd * p + co * beside, csd * p + cso * beside

    def columns_rows(q, carry):
        for i in range(4):
            r = q * 4 + i
            u, v = columns(xs[r], geno * FR + r)
            us[r + 1] = u
            vs[r + 1] = v
        return carry

    lax.fori_loop(0, FR // 4, columns_rows, 0)

    pl.semaphore_wait(barrier, DEVICES - 1)
    above = (trial, lax.rem(geno + 3, 4))
    below = (trial, lax.rem(geno + 1, 4))
    edges = [
        pltpu.make_async_remote_copy(
            src_ref=xs.at[0], dst_ref=halo.at[1], send_sem=halo_send.at[0],
            recv_sem=halo_recv.at[1], device_id=above, device_id_type=MESH,
        ),
        pltpu.make_async_remote_copy(
            src_ref=xs.at[FR - 1], dst_ref=halo.at[0], send_sem=halo_send.at[1],
            recv_sem=halo_recv.at[0], device_id=below, device_id_type=MESH,
        ),
    ]
    for edge in edges:
        edge.start()

    def terms_row(r):
        row = geno * FR + r
        edge = (row == 0) | (row == n_rows - 1)
        rd = jnp.where(edge, re, ri)
        rsd = jnp.where(edge, rse, rsi)
        present = in_col & (row < n_rows)
        k0, k1, k2 = [jnp.where(present, gain, F32(0)) for gain in gains]
        u, v = us[r + 1], vs[r + 1]
        u2 = us[r] + us[r + 2]
        v2 = vs[r] + vs[r + 2]
        values = [
            (rd * u + ro * u2) * k0,
            (rsd * u + rso * u2) * k1,
            (rd * v + ro * v2) * k2,
        ]
        words = []
        for value in values:
            q = jnp.floor(value + 0.5).astype(I32)
            words.append((q[8:] << 16) | (q[:8] & 0xFFFF))
        aux = jnp.where(sub8 < PER_ROW, slot_ref[r], scale_rows)
        stacked = jnp.concatenate(words * PER_ROW + [aux], axis=0)
        table[pl.ds(pl.multiple_of((r + 1) * FC, FC), FC), :] = stacked.T

    def inner_rows(q, carry):
        for i in range(TERM_ROWS):
            terms_row(1 + q * TERM_ROWS + i)
        return carry

    lax.fori_loop(0, (FR - 2) // TERM_ROWS, inner_rows, 0)
    for edge in edges:
        edge.wait()
    for side, r in ((0, -1), (1, FR)):
        row = jnp.where((geno == 0) & (side == 0), -1, geno * FR + r)
        u, v = columns(halo[side], row)
        us[r + 1] = u
        vs[r + 1] = v

    def outer_row(i, carry):
        terms_row(i * (FR - 1))
        return carry

    lax.fori_loop(0, 2, outer_row, 0)
    to_smem.wait()

    def gather(target, dst):
        for r in range(ROWS):
            row = None
            for j in range(PER_ROW):
                place = min(r * PER_ROW + j, SLOTS - 1)
                part = table[pl.ds(picks_s.at[place][target], 1), :]
                if r * PER_ROW + j >= SLOTS:
                    part = table[0:1, :]
                row = part if row is None else jnp.where(masks[j], part, row)
            dst[pl.ds(r, 1), :] = row

    def copy_of(s, target=None):
        return pltpu.make_async_remote_copy(
            src_ref=sbuf.at[s], dst_ref=rbuf.at[s, pl.ds(0, ROWS)],
            send_sem=send_sem.at[s], recv_sem=recv_sem.at[s],
            device_id=below if target is None else target, device_id_type=MESH,
        )

    acc[...] = jnp.zeros_like(acc)

    def fill(step, last):
        for i in range(4):
            s = step * 4 + i
            target = shifted(step, i)
            gather(target[0] * 4 + target[1], sbuf.at[s])
            if i < 2:

                @pl.when(step > 0)
                def _(s=s, last=last):
                    copy_of(s - 1, last).start()

            else:
                copy_of(s - 1, last).start()
            last = target
        return last

    width = BATCH * PAD_ROWS
    high_id = lax.broadcasted_iota(I32, (FC, width), 0)
    pos = lax.rem(lax.broadcasted_iota(I32, (1, width), 1), PAD_ROWS)

    def add_batch(b):
        def arrive(s, carry):
            copy_of(s).wait()
            return carry

        lax.fori_loop(jnp.maximum(b * BATCH, 1), (b + 1) * BATCH, arrive, 0)
        block = rbuf[pl.ds(b * BATCH, BATCH)].reshape(width, 128).T
        scales = [
            block[125 + t : 126 + t, :].astype(F32) * (1.0 / (float(1 << SCALE_BITS) * 32766.0))
            for t in range(3)
        ]
        total = acc[...]
        for j in range(PER_ROW):
            slot = jnp.where(pos < ROWS, block[120 + j : 121 + j, :], -1)
            low = slot >> 8
            hot = jnp.where(high_id == (slot & 255), F32(1), F32(0)).astype(BF16)
            parts = []
            for t in range(3):
                word = block[(j * 3 + t) * 8 : (j * 3 + t + 1) * 8, :]
                parts.append(((word << 16) >> 16).astype(F32) * scales[t])
                parts.append((word >> 16).astype(F32) * scales[t])
            values = jnp.concatenate(parts, axis=0)
            split = jnp.concatenate(
                [jnp.where(low == q, values, F32(0)) for q in range(4)], axis=0
            ).astype(BF16)
            total = total + lax.dot_general(
                split, hot, (((1,), (1,)), ((), ())), preferred_element_type=F32
            )
        acc[...] = total

    def stage(b, last):
        last = lax.fori_loop(b * 4, b * 4 + 4, fill, last)

        @pl.when(b == 0)
        def _():
            rbuf[0, 0:ROWS, :] = sbuf[0]

        @pl.when(b >= 2)
        def _():
            add_batch(b - 2)

        return last

    last = lax.fori_loop(0, BATCHES, stage, (trial, geno))
    copy_of(DEVICES - 1, last).start()

    def tail(b, carry):
        add_batch(b)
        return carry

    lax.fori_loop(BATCHES - 2, BATCHES, tail, 0)
    for q in range(4):
        out_ref[:, q * FC : (q + 1) * FC] = acc[q * 48 : (q + 1) * 48, :]


def body(probe_signs, trial_rows, trial_cols, ar_rho, res_var, plot_owner, plot_slot):
    smem = pl.BlockSpec(memory_space=pltpu.SMEM)
    vmem = pl.BlockSpec(memory_space=pltpu.VMEM)
    out = pl.pallas_call(
        kernel,
        out_shape=jax.ShapeDtypeStruct((3 * PROBES, G_DEV), F32),
        in_specs=[pl.BlockSpec(memory_space=pl.ANY), smem, smem, smem, smem, vmem, vmem],
        out_specs=vmem,
        scratch_shapes=[
            pltpu.VMEM((FR, PROBES, FC), I32),
            pltpu.VMEM((FR + 2, PROBES, FC), F32),
            pltpu.VMEM((FR + 2, PROBES, FC), F32),
            pltpu.VMEM((2, PROBES, FC), I32),
            pltpu.VMEM(((FR + 1) * FC, 128), I32),
            pltpu.VMEM((SLOTS, DEVICES), I32),
            pltpu.SMEM((SLOTS, DEVICES), I32),
            pltpu.VMEM((DEVICES, ROWS, 128), I32),
            pltpu.VMEM((DEVICES, PAD_ROWS, 128), I32),
            pltpu.VMEM((SLOTS, 2 * DEVICES), F32),
            pltpu.VMEM((12 * PROBES, FC), F32),
            pltpu.SemaphoreType.DMA((PROBES,)),
            pltpu.SemaphoreType.DMA,
            pltpu.SemaphoreType.DMA((2,)),
            pltpu.SemaphoreType.DMA((2,)),
            pltpu.SemaphoreType.DMA((DEVICES,)),
            pltpu.SemaphoreType.DMA((DEVICES,)),
        ],
        compiler_params=pltpu.CompilerParams(
            collective_id=0, has_side_effects=True, vmem_limit_bytes=56 << 20
        ),
        name="hutchinson_exchange",
    )(
        probe_signs.transpose(0, 1, 3, 2, 4).reshape(PROBES, FR, 1, FC),
        trial_rows,
        trial_cols,
        ar_rho,
        res_var,
        plot_owner.transpose(0, 1, 2, 4, 3).reshape(FR, 1, FC),
        plot_slot.transpose(0, 2, 1, 3).reshape(FR, 1, FC),
    )
    return out.reshape(3, PROBES, G_DEV)


def solution(mesh):
    return jax.shard_map(
        body,
        mesh=mesh,
        in_specs=(
            P(None, ("trial", "geno"), None, None, None),
            P("trial"),
            P("trial"),
            P("trial", None),
            P("trial"),
            P(("trial", "geno"), None, None, None, None),
            P(("trial", "geno"), None, None, None),
        ),
        out_specs=P(None, None, ("trial", "geno")),
        check_vma=False,
    )
```

```python
import jax
import jax.numpy as jnp
from jax import lax
from jax.experimental import pallas as pl
from jax.experimental.pallas import tpu as pltpu
from jax.sharding import PartitionSpec as P

G_DEV = 1024
PROBES = 16
FR = 44
FC = 256
DEVICES = 128
PER_ROW = 5
WORDS = 24
SLOTS = 176
ROWS = 36
PAD_ROWS = 40
BATCH = 16
BATCHES = DEVICES // BATCH
RANK_ROWS = 22
TERM_ROWS = 7
SCALE_BITS = 24
MESH = pl.DeviceIdType.MESH
F32 = jnp.float32
BF16 = jnp.bfloat16
I32 = jnp.int32


def places():
    trial, geno = lax.axis_index("trial"), lax.axis_index("geno")
    return trial // 8, lax.rem(trial // 2, 4), lax.rem(trial, 2), geno


def shifted(step, i):
    z, y, core, x = places()
    far = step // 4
    near = lax.rem(step, 4)
    tz = lax.rem(z + lax.rem(far, 4) + 2 * near + i, 4)
    ty = lax.rem(y + near, 4)
    tc = lax.rem(core + far // 4 + near + i // 2, 2)
    return tz * 8 + ty * 2 + tc, lax.rem(x + i, 4)


def kernel(
    signs_ref, rows_ref, cols_ref, rho_ref, var_ref, owner_ref, slot_ref, out_ref,
    owners, slots, xs, us, vs, halo, table, picks, picks_s, sbuf, rbuf, digits, acc,
    in_sem, pick_sem, halo_send, halo_recv, send_sem, recv_sem,
):
    trial, geno = lax.axis_index("trial"), lax.axis_index("geno")
    barrier = pltpu.get_barrier_semaphore()

    loads = [
        pltpu.make_async_copy(signs_ref.at[p, :, 0], xs.at[:, p, :], in_sem.at[p])
        for p in range(PROBES)
    ]
    owner_load = pltpu.make_async_copy(owner_ref, owners, in_sem.at[PROBES])
    slot_load = pltpu.make_async_copy(slot_ref, slots, in_sem.at[PROBES + 1])
    for load in [owner_load, *loads, slot_load]:
        load.start()

    def signal(step, i):
        pl.semaphore_signal(barrier, inc=1, device_id=shifted(step, i), device_id_type=MESH)

    def greet(step, carry):
        for i in range(4):
            signal(step, i)
        return carry

    for i in range(1, 4):
        signal(0, i)
    lax.fori_loop(1, DEVICES // 4, greet, 0)

    def tall(row, height):
        row = jnp.broadcast_to(row, (16, row.shape[1])).astype(F32).astype(BF16)
        return jnp.concatenate([row] * (height // 16), axis=0)

    def ids(height, width):
        return lax.broadcasted_iota(I32, (height, width), 0).astype(F32).astype(BF16)

    one, none = BF16(1), BF16(0)
    owner_id = ids(DEVICES, FC)
    place_id = ids(SLOTS, FC)
    col_i = lax.broadcasted_iota(I32, (FC, FC), 0)
    col_j = lax.broadcasted_iota(I32, (FC, FC), 1)
    upto = jnp.where(col_i <= col_j, F32(1), F32(0)).astype(BF16)
    col_no = tall(lax.broadcasted_iota(I32, (1, FC), 1), DEVICES)
    digits[...] = jnp.zeros_like(digits)
    owner_load.wait()

    def rank_rows(q, running):
        owns = [owner_id == tall(owners[q * RANK_ROWS + i], DEVICES) for i in range(RANK_ROWS)]
        hots = jnp.concatenate([jnp.where(own, one, none) for own in owns], axis=0)
        counts = jnp.dot(hots, upto, preferred_element_type=F32)
        lefts, rights = [], []
        for i, own in enumerate(owns):
            count = counts[i * DEVICES : (i + 1) * DEVICES]
            before = jnp.concatenate([running.astype(BF16)] * 2, axis=1)
            running = running + jnp.broadcast_to(count[:, FC - 1 :], (DEVICES, 128))
            mine = jnp.where(own, count.astype(BF16) + before, none)
            parts = [mine[j * 16 : (j + 1) * 16] for j in range(DEVICES // 16)]
            while len(parts) > 1:
                parts = [x + y for x, y in zip(parts[::2], parts[1::2])]
            place = jnp.sum(parts[0].astype(F32), axis=0, keepdims=True) - 1.0
            lefts.append(jnp.where(place_id == tall(place, SLOTS), one, none))
            row_no = tall(jnp.full((1, FC), q * RANK_ROWS + i + 1, I32), DEVICES)
            rights.append(
                jnp.concatenate([jnp.where(own, row_no, none), jnp.where(own, col_no, none)], axis=0)
            )
        digits[...] += lax.dot_general(
            jnp.concatenate(lefts, axis=1), jnp.concatenate(rights, axis=1),
            (((1,), (1,)), ((), ())), preferred_element_type=F32,
        )
        return running

    lax.fori_loop(0, FR // RANK_ROWS, rank_rows, jnp.zeros((DEVICES, 128), F32))
    plot = (digits[:, :DEVICES] * float(FC) + digits[:, DEVICES:]).astype(I32)
    picks[...] = jnp.clip(plot, 0, (FR + 1) * FC - 1)
    to_smem = pltpu.make_async_copy(picks, picks_s, pick_sem)
    to_smem.start()

    n_rows, n_cols = rows_ref[0], cols_ref[0]
    rho_r = jnp.full((1, FC), rho_ref[0, 0], F32)
    rho_c = jnp.full((1, FC), rho_ref[0, 1], F32)
    res = jnp.full((1, FC), var_ref[0], F32)
    col = lax.broadcasted_iota(I32, (1, FC), 1)

    def line(rho):
        inv = 1.0 / (1.0 - rho * rho)
        inside = 1.0 + rho * rho
        return (
            (inv, inv * inside, -inv * rho),
            (2.0 * rho * inv * inv, 4.0 * rho * inv * inv, -inside * inv * inv),
        )

    (ce, ci, co), (cse, csi, cso) = line(rho_c)
    (re, ri, ro), (rse, rsi, rso) = line(rho_r)
    col_edge = (col == 0) | (col == n_cols - 1)
    cd = jnp.where(col_edge, ce, ci)
    csd = jnp.where(col_edge, cse, csi)
    in_col = col < n_cols
    left_ok = col > 0
    right_ok = col < FC - 1
    inv_res = 1.0 / res
    c_top = jnp.maximum(ce, ci) - 2.0 * co
    cs_top = jnp.maximum(cse, csi) - 2.0 * cso
    r_top = jnp.maximum(re, ri) - 2.0 * ro
    rs_top = jnp.maximum(rse, rsi) - 2.0 * rso
    tops = [r_top * c_top * inv_res, rs_top * c_top * inv_res, r_top * cs_top * inv_res]
    scale_ints = [jnp.ceil(top * float(1 << SCALE_BITS)).astype(I32) + 1 for top in tops]
    gains = [
        inv_res * 32766.0 / (s.astype(F32) * (1.0 / float(1 << SCALE_BITS))) for s in scale_ints
    ]
    sub8 = lax.broadcasted_iota(I32, (8, FC), 0)
    scale_rows = jnp.where(
        sub8 == 5, scale_ints[0], jnp.where(sub8 == 6, scale_ints[1], scale_ints[2])
    )

    lane = lax.broadcasted_iota(I32, (1, 128), 1)
    group = jnp.where(lane < PER_ROW * WORDS, lane // WORDS, lane - PER_ROW * WORDS)
    group = jnp.where(group >= PER_ROW, 0, group)
    masks = [group == j for j in range(PER_ROW)]
    lane8 = lax.broadcasted_iota(I32, (8, 128), 1)
    first_scales = jnp.where(
        lane8 == 125, scale_ints[0][:, :128],
        jnp.where(lane8 == 126, scale_ints[1][:, :128], scale_ints[2][:, :128]),
    )
    table[0:8, :] = jnp.where(lane8 >= 125, first_scales, jnp.where(lane8 >= 120, -1, 0))

    for load in [*loads, slot_load]:
        load.wait()

    def columns(bits, row):
        present = in_col & (row >= 0) & (row < n_rows)
        p = jnp.where(present, 2.0 * bits.astype(F32) - 1.0, F32(0))
        beside = jnp.where(left_ok, pltpu.roll(p, 1, 1), F32(0)) + jnp.where(
            right_ok, pltpu.roll(p, FC - 1, 1), F32(0)
        )
        return cd * p + co * beside, csd * p + cso * beside

    def columns_rows(q, carry):
        for i in range(4):
            r = q * 4 + i
            u, v = columns(xs[r], geno * FR + r)
            us[r + 1] = u
            vs[r + 1] = v
        return carry

    lax.fori_loop(0, FR // 4, columns_rows, 0)

    pl.semaphore_wait(barrier, DEVICES - 1)
    above = (trial, lax.rem(geno + 3, 4))
    below = (trial, lax.rem(geno + 1, 4))
    edges = [
        pltpu.make_async_remote_copy(
            src_ref=xs.at[0], dst_ref=halo.at[1], send_sem=halo_send.at[0],
            recv_sem=halo_recv.at[1], device_id=above, device_id_type=MESH,
        ),
        pltpu.make_async_remote_copy(
            src_ref=xs.at[FR - 1], dst_ref=halo.at[0], send_sem=halo_send.at[1],
            recv_sem=halo_recv.at[0], device_id=below, device_id_type=MESH,
        ),
    ]
    for edge in edges:
        edge.start()

    def terms_row(r):
        row = geno * FR + r
        edge = (row == 0) | (row == n_rows - 1)
        rd = jnp.where(edge, re, ri)
        rsd = jnp.where(edge, rse, rsi)
        present = in_col & (row < n_rows)
        k0, k1, k2 = [jnp.where(present, gain, F32(0)) for gain in gains]
        u, v = us[r + 1], vs[r + 1]
        u2 = us[r] + us[r + 2]
        v2 = vs[r] + vs[r + 2]
        values = [
            (rd * u + ro * u2) * k0,
            (rsd * u + rso * u2) * k1,
            (rd * v + ro * v2) * k2,
        ]
        words = []
        for value in values:
            q = jnp.floor(value + 0.5).astype(I32)
            words.append((q[8:] << 16) | (q[:8] & 0xFFFF))
        aux = jnp.where(sub8 < PER_ROW, slots[r], scale_rows)
        stacked = jnp.concatenate(words * PER_ROW + [aux], axis=0)
        table[pl.ds(pl.multiple_of((r + 1) * FC, FC), FC), :] = stacked.T

    def inner_rows(q, carry):
        for i in range(TERM_ROWS):
            terms_row(1 + q * TERM_ROWS + i)
        return carry

    lax.fori_loop(0, (FR - 2) // TERM_ROWS, inner_rows, 0)
    for edge in edges:
        edge.wait()
    for side, r in ((0, -1), (1, FR)):
        row = jnp.where((geno == 0) & (side == 0), -1, geno * FR + r)
        u, v = columns(halo[side], row)
        us[r + 1] = u
        vs[r + 1] = v

    def outer_row(i, carry):
        terms_row(i * (FR - 1))
        return carry

    lax.fori_loop(0, 2, outer_row, 0)
    to_smem.wait()

    def gather(target, dst):
        for r in range(ROWS):
            row = None
            for j in range(PER_ROW):
                place = min(r * PER_ROW + j, SLOTS - 1)
                part = table[pl.ds(picks_s.at[place][target], 1), :]
                if r * PER_ROW + j >= SLOTS:
                    part = table[0:1, :]
                row = part if row is None else jnp.where(masks[j], part, row)
            dst[pl.ds(r, 1), :] = row

    def copy_of(s, target=None):
        return pltpu.make_async_remote_copy(
            src_ref=sbuf.at[s], dst_ref=rbuf.at[s, pl.ds(0, ROWS)],
            send_sem=send_sem.at[s], recv_sem=recv_sem.at[s],
            device_id=below if target is None else target, device_id_type=MESH,
        )

    acc[...] = jnp.zeros_like(acc)

    def fill(step, last):
        for i in range(4):
            s = step * 4 + i
            target = shifted(step, i)
            gather(target[0] * 4 + target[1], sbuf.at[s])
            if i < 2:

                @pl.when(step > 0)
                def _(s=s, last=last):
                    copy_of(s - 1, last).start()

            else:
                copy_of(s - 1, last).start()
            last = target
        return last

    width = BATCH * PAD_ROWS
    high_id = ids(FC, width)
    pos = lax.rem(lax.broadcasted_iota(I32, (1, width), 1), PAD_ROWS)

    def add_batch(b):
        def arrive(s, carry):
            copy_of(s).wait()
            return carry

        lax.fori_loop(jnp.maximum(b * BATCH, 1), (b + 1) * BATCH, arrive, 0)
        block = rbuf[pl.ds(b * BATCH, BATCH)].reshape(width, 128).T
        scales = [
            block[125 + t : 126 + t, :].astype(F32) * (1.0 / (float(1 << SCALE_BITS) * 32766.0))
            for t in range(3)
        ]
        splits, hots = [], []
        for j in range(PER_ROW):
            slot = jnp.where(pos < ROWS, block[120 + j : 121 + j, :], -1)
            low = slot >> 8
            hots.append(jnp.where(high_id == tall(slot & 255, FC), one, none))
            parts = []
            for t in range(3):
                word = block[(j * 3 + t) * 8 : (j * 3 + t + 1) * 8, :]
                parts.append(((word << 16) >> 16).astype(F32) * scales[t])
                parts.append((word >> 16).astype(F32) * scales[t])
            values = jnp.concatenate(parts, axis=0).astype(BF16)
            low = tall(low, 48)
            splits.append(
                jnp.concatenate([jnp.where(low == BF16(q), values, none) for q in range(4)], axis=0)
            )
        acc[...] += lax.dot_general(
            jnp.concatenate(splits, axis=1), jnp.concatenate(hots, axis=1),
            (((1,), (1,)), ((), ())), preferred_element_type=F32,
        )

    def stage(b, last):
        last = lax.fori_loop(b * 4, b * 4 + 4, fill, last)

        @pl.when(b == 0)
        def _():
            rbuf[0, 0:ROWS, :] = sbuf[0]

        @pl.when(b >= 2)
        def _():
            add_batch(b - 2)

        return last

    last = lax.fori_loop(0, BATCHES, stage, (trial, geno))
    copy_of(DEVICES - 1, last).start()

    def tail(b, carry):
        add_batch(b)
        return carry

    lax.fori_loop(BATCHES - 2, BATCHES, tail, 0)
    for q in range(4):
        out_ref[:, q * FC : (q + 1) * FC] = acc[q * 48 : (q + 1) * 48, :]


def body(probe_signs, trial_rows, trial_cols, ar_rho, res_var, plot_owner, plot_slot):
    smem = pl.BlockSpec(memory_space=pltpu.SMEM)
    vmem = pl.BlockSpec(memory_space=pltpu.VMEM)
    hbm = pl.BlockSpec(memory_space=pl.ANY)
    out = pl.pallas_call(
        kernel,
        out_shape=jax.ShapeDtypeStruct((3 * PROBES, G_DEV), F32),
        in_specs=[hbm, smem, smem, smem, smem, hbm, hbm],
        out_specs=vmem,
        scratch_shapes=[
            pltpu.VMEM((FR, 1, FC), I32),
            pltpu.VMEM((FR, 1, FC), I32),
            pltpu.VMEM((FR, PROBES, FC), I32),
            pltpu.VMEM((FR + 2, PROBES, FC), F32),
            pltpu.VMEM((FR + 2, PROBES, FC), F32),
            pltpu.VMEM((2, PROBES, FC), I32),
            pltpu.VMEM(((FR + 1) * FC, 128), I32),
            pltpu.VMEM((SLOTS, DEVICES), I32),
            pltpu.SMEM((SLOTS, DEVICES), I32),
            pltpu.VMEM((DEVICES, ROWS, 128), I32),
            pltpu.VMEM((DEVICES, PAD_ROWS, 128), I32),
            pltpu.VMEM((SLOTS, 2 * DEVICES), F32),
            pltpu.VMEM((12 * PROBES, FC), F32),
            pltpu.SemaphoreType.DMA((PROBES + 2,)),
            pltpu.SemaphoreType.DMA,
            pltpu.SemaphoreType.DMA((2,)),
            pltpu.SemaphoreType.DMA((2,)),
            pltpu.SemaphoreType.DMA((DEVICES,)),
            pltpu.SemaphoreType.DMA((DEVICES,)),
        ],
        compiler_params=pltpu.CompilerParams(
            collective_id=0, has_side_effects=True, vmem_limit_bytes=56 << 20
        ),
        name="hutchinson_exchange",
    )(
        probe_signs.transpose(0, 1, 3, 2, 4).reshape(PROBES, FR, 1, FC),
        trial_rows,
        trial_cols,
        ar_rho,
        res_var,
        plot_owner.transpose(0, 1, 2, 4, 3).reshape(FR, 1, FC),
        plot_slot.transpose(0, 2, 1, 3).reshape(FR, 1, FC),
    )
    return out.reshape(3, PROBES, G_DEV)


def solution(mesh):
    return jax.shard_map(
        body,
        mesh=mesh,
        in_specs=(
            P(None, ("trial", "geno"), None, None, None),
            P("trial"),
            P("trial"),
            P("trial", None),
            P("trial"),
            P(("trial", "geno"), None, None, None, None),
            P(("trial", "geno"), None, None, None),
        ),
        out_specs=P(None, None, ("trial", "geno")),
        check_vma=False,
    )
```

```python
import jax
import jax.numpy as jnp
from jax import lax
from jax.experimental import pallas as pl
from jax.experimental.pallas import tpu as pltpu
from jax.sharding import PartitionSpec as P

G_DEV = 1024
PROBES = 16
FR = 44
FC = 256
DEVICES = 128
PER_ROW = 5
WORDS = 24
SLOTS = 176
ROWS = 36
PAD_ROWS = 40
BATCH = 16
BATCHES = DEVICES // BATCH
RANK_ROWS = 22
TERM_ROWS = 7
SCALE_BITS = 24
MESH = pl.DeviceIdType.MESH
F32 = jnp.float32
BF16 = jnp.bfloat16
I32 = jnp.int32


def send_order():
    shifts = [(k % 4, k // 4 % 4, k // 16 % 4, k // 64) for k in range(1, DEVICES)]
    mixed = [shifts[(i * 50 + 13) % (DEVICES - 1)] for i in range(DEVICES - 1)]
    return sorted(mixed, key=lambda d: -sum(min(d[a], 4 - d[a]) for a in range(3)))


def kernel(
    signs_ref, rows_ref, cols_ref, rho_ref, var_ref, owner_ref, slot_ref, out_ref,
    trials, genos, owners, slots, xs, us, vs, halo, table, picks, picks_s, sbuf, rbuf, digits, acc,
    in_sem, pick_sem, halo_send, halo_recv, send_sem, recv_sem,
):
    trial, geno = lax.axis_index("trial"), lax.axis_index("geno")
    barrier = pltpu.get_barrier_semaphore()

    loads = [
        pltpu.make_async_copy(signs_ref.at[p, :, 0], xs.at[:, p, :], in_sem.at[p])
        for p in range(PROBES)
    ]
    owner_load = pltpu.make_async_copy(owner_ref, owners, in_sem.at[PROBES])
    slot_load = pltpu.make_async_copy(slot_ref, slots, in_sem.at[PROBES + 1])
    for load in [owner_load, *loads, slot_load]:
        load.start()

    z, y, core = trial // 8, lax.rem(trial // 2, 4), lax.rem(trial, 2)
    xs_at = [lax.rem(geno + i, 4) for i in range(4)]
    ys_at = [lax.rem(y + i, 4) * 2 for i in range(4)]
    zs_at = [lax.rem(z + i, 4) * 8 for i in range(4)]
    cores_at = [core, 1 - core]
    trials[0] = trial
    genos[0] = geno
    for s, (dx, dy, dz, dc) in enumerate(send_order(), 1):
        t, g = zs_at[dz] + ys_at[dy] + cores_at[dc], xs_at[dx]
        pl.semaphore_signal(barrier, inc=1, device_id=(t, g), device_id_type=MESH)
        trials[s] = t
        genos[s] = g

    def tall(row, height):
        row = jnp.broadcast_to(row, (16, row.shape[1])).astype(F32).astype(BF16)
        return jnp.concatenate([row] * (height // 16), axis=0)

    def ids(height, width):
        return lax.broadcasted_iota(I32, (height, width), 0).astype(F32).astype(BF16)

    one, none = BF16(1), BF16(0)
    owner_id = ids(DEVICES, FC)
    place_id = ids(SLOTS, FC)
    col_i = lax.broadcasted_iota(I32, (FC, FC), 0)
    col_j = lax.broadcasted_iota(I32, (FC, FC), 1)
    upto = jnp.where(col_i <= col_j, F32(1), F32(0)).astype(BF16)
    col_no = tall(lax.broadcasted_iota(I32, (1, FC), 1), DEVICES)
    digits[...] = jnp.zeros_like(digits)
    owner_load.wait()

    def rank_rows(q, running):
        owns = [owner_id == tall(owners[q * RANK_ROWS + i], DEVICES) for i in range(RANK_ROWS)]
        hots = jnp.concatenate([jnp.where(own, one, none) for own in owns], axis=0)
        counts = jnp.dot(hots, upto, preferred_element_type=F32)
        lefts, rights = [], []
        for i, own in enumerate(owns):
            count = counts[i * DEVICES : (i + 1) * DEVICES]
            before = jnp.concatenate([running.astype(BF16)] * 2, axis=1)
            running = running + jnp.broadcast_to(count[:, FC - 1 :], (DEVICES, 128))
            mine = jnp.where(own, count.astype(BF16) + before, none)
            parts = [mine[j * 16 : (j + 1) * 16] for j in range(DEVICES // 16)]
            while len(parts) > 1:
                parts = [x + y for x, y in zip(parts[::2], parts[1::2])]
            place = jnp.sum(parts[0].astype(F32), axis=0, keepdims=True) - 1.0
            lefts.append(jnp.where(place_id == tall(place, SLOTS), one, none))
            row_no = tall(jnp.full((1, FC), q * RANK_ROWS + i + 1, I32), DEVICES)
            rights.append(
                jnp.concatenate([jnp.where(own, row_no, none), jnp.where(own, col_no, none)], axis=0)
            )
        digits[...] += lax.dot_general(
            jnp.concatenate(lefts, axis=1), jnp.concatenate(rights, axis=1),
            (((1,), (1,)), ((), ())), preferred_element_type=F32,
        )
        return running

    lax.fori_loop(0, FR // RANK_ROWS, rank_rows, jnp.zeros((DEVICES, 128), F32))
    plot = (digits[:, :DEVICES] * float(FC) + digits[:, DEVICES:]).astype(I32)
    picks[...] = jnp.clip(plot, 0, (FR + 1) * FC - 1)
    to_smem = pltpu.make_async_copy(picks, picks_s, pick_sem)
    to_smem.start()

    n_rows, n_cols = rows_ref[0], cols_ref[0]
    rho_r = jnp.full((1, FC), rho_ref[0, 0], F32)
    rho_c = jnp.full((1, FC), rho_ref[0, 1], F32)
    res = jnp.full((1, FC), var_ref[0], F32)
    col = lax.broadcasted_iota(I32, (1, FC), 1)

    def line(rho):
        inv = 1.0 / (1.0 - rho * rho)
        inside = 1.0 + rho * rho
        return (
            (inv, inv * inside, -inv * rho),
            (2.0 * rho * inv * inv, 4.0 * rho * inv * inv, -inside * inv * inv),
        )

    (ce, ci, co), (cse, csi, cso) = line(rho_c)
    (re, ri, ro), (rse, rsi, rso) = line(rho_r)
    col_edge = (col == 0) | (col == n_cols - 1)
    cd = jnp.where(col_edge, ce, ci)
    csd = jnp.where(col_edge, cse, csi)
    in_col = col < n_cols
    left_ok = col > 0
    right_ok = col < FC - 1
    inv_res = 1.0 / res
    c_top = jnp.maximum(ce, ci) - 2.0 * co
    cs_top = jnp.maximum(cse, csi) - 2.0 * cso
    r_top = jnp.maximum(re, ri) - 2.0 * ro
    rs_top = jnp.maximum(rse, rsi) - 2.0 * rso
    tops = [r_top * c_top * inv_res, rs_top * c_top * inv_res, r_top * cs_top * inv_res]
    scale_ints = [jnp.ceil(top * float(1 << SCALE_BITS)).astype(I32) + 1 for top in tops]
    gains = [
        inv_res * 32766.0 / (s.astype(F32) * (1.0 / float(1 << SCALE_BITS))) for s in scale_ints
    ]
    sub8 = lax.broadcasted_iota(I32, (8, FC), 0)
    scale_rows = jnp.where(
        sub8 == 5, scale_ints[0], jnp.where(sub8 == 6, scale_ints[1], scale_ints[2])
    )

    lane = lax.broadcasted_iota(I32, (1, 128), 1)
    group = jnp.where(lane < PER_ROW * WORDS, lane // WORDS, lane - PER_ROW * WORDS)
    group = jnp.where(group >= PER_ROW, 0, group)
    masks = [group == j for j in range(PER_ROW)]
    lane8 = lax.broadcasted_iota(I32, (8, 128), 1)
    first_scales = jnp.where(
        lane8 == 125, scale_ints[0][:, :128],
        jnp.where(lane8 == 126, scale_ints[1][:, :128], scale_ints[2][:, :128]),
    )
    table[0:8, :] = jnp.where(lane8 >= 125, first_scales, jnp.where(lane8 >= 120, -1, 0))

    for load in [*loads, slot_load]:
        load.wait()

    def columns(bits, row):
        present = in_col & (row >= 0) & (row < n_rows)
        p = jnp.where(present, 2.0 * bits.astype(F32) - 1.0, F32(0))
        beside = jnp.where(left_ok, pltpu.roll(p, 1, 1), F32(0)) + jnp.where(
            right_ok, pltpu.roll(p, FC - 1, 1), F32(0)
        )
        return cd * p + co * beside, csd * p + cso * beside

    def columns_rows(q, carry):
        for i in range(4):
            r = q * 4 + i
            u, v = columns(xs[r], geno * FR + r)
            us[r + 1] = u
            vs[r + 1] = v
        return carry

    lax.fori_loop(0, FR // 4, columns_rows, 0)

    pl.semaphore_wait(barrier, DEVICES - 1)
    above = (trial, lax.rem(geno + 3, 4))
    below = (trial, lax.rem(geno + 1, 4))
    edges = [
        pltpu.make_async_remote_copy(
            src_ref=xs.at[0], dst_ref=halo.at[1], send_sem=halo_send.at[0],
            recv_sem=halo_recv.at[1], device_id=above, device_id_type=MESH,
        ),
        pltpu.make_async_remote_copy(
            src_ref=xs.at[FR - 1], dst_ref=halo.at[0], send_sem=halo_send.at[1],
            recv_sem=halo_recv.at[0], device_id=below, device_id_type=MESH,
        ),
    ]
    for edge in edges:
        edge.start()

    def terms_row(r):
        row = geno * FR + r
        edge = (row == 0) | (row == n_rows - 1)
        rd = jnp.where(edge, re, ri)
        rsd = jnp.where(edge, rse, rsi)
        present = in_col & (row < n_rows)
        k0, k1, k2 = [jnp.where(present, gain, F32(0)) for gain in gains]
        u, v = us[r + 1], vs[r + 1]
        u2 = us[r] + us[r + 2]
        v2 = vs[r] + vs[r + 2]
        values = [
            (rd * u + ro * u2) * k0,
            (rsd * u + rso * u2) * k1,
            (rd * v + ro * v2) * k2,
        ]
        words = []
        for value in values:
            q = jnp.floor(value + 0.5).astype(I32)
            words.append((q[8:] << 16) | (q[:8] & 0xFFFF))
        aux = jnp.where(sub8 < PER_ROW, slots[r], scale_rows)
        stacked = jnp.concatenate(words * PER_ROW + [aux], axis=0)
        table[pl.ds(pl.multiple_of((r + 1) * FC, FC), FC), :] = stacked.T

    def inner_rows(q, carry):
        for i in range(TERM_ROWS):
            terms_row(1 + q * TERM_ROWS + i)
        return carry

    lax.fori_loop(0, (FR - 2) // TERM_ROWS, inner_rows, 0)
    for edge in edges:
        edge.wait()
    for side, r in ((0, -1), (1, FR)):
        row = jnp.where((geno == 0) & (side == 0), -1, geno * FR + r)
        u, v = columns(halo[side], row)
        us[r + 1] = u
        vs[r + 1] = v

    def outer_row(i, carry):
        terms_row(i * (FR - 1))
        return carry

    lax.fori_loop(0, 2, outer_row, 0)
    to_smem.wait()

    def gather(target, dst):
        for r in range(ROWS):
            row = None
            for j in range(PER_ROW):
                place = min(r * PER_ROW + j, SLOTS - 1)
                part = table[pl.ds(picks_s.at[place][target], 1), :]
                if r * PER_ROW + j >= SLOTS:
                    part = table[0:1, :]
                row = part if row is None else jnp.where(masks[j], part, row)
            dst[pl.ds(r, 1), :] = row

    def copy_of(s, target=None):
        return pltpu.make_async_remote_copy(
            src_ref=sbuf.at[s], dst_ref=rbuf.at[s, pl.ds(0, ROWS)],
            send_sem=send_sem.at[s], recv_sem=recv_sem.at[s],
            device_id=below if target is None else target, device_id_type=MESH,
        )

    acc[...] = jnp.zeros_like(acc)

    def fill(step, last):
        for i in range(4):
            s = step * 4 + i
            target = trials[s], genos[s]
            gather(target[0] * 4 + target[1], sbuf.at[s])
            if i < 2:

                @pl.when(step > 0)
                def _(s=s, last=last):
                    copy_of(s - 1, last).start()

            else:
                copy_of(s - 1, last).start()
            last = target
        return last

    width = BATCH * PAD_ROWS
    high_id = ids(FC, width)
    pos = lax.rem(lax.broadcasted_iota(I32, (1, width), 1), PAD_ROWS)

    def add_batch(b):
        def arrive(s, carry):
            copy_of(s).wait()
            return carry

        lax.fori_loop(jnp.maximum(b * BATCH, 1), (b + 1) * BATCH, arrive, 0)
        block = rbuf[pl.ds(b * BATCH, BATCH)].reshape(width, 128).T
        scales = [
            block[125 + t : 126 + t, :].astype(F32) * (1.0 / (float(1 << SCALE_BITS) * 32766.0))
            for t in range(3)
        ]
        splits, hots = [], []
        for j in range(PER_ROW):
            slot = jnp.where(pos < ROWS, block[120 + j : 121 + j, :], -1)
            low = slot >> 8
            hots.append(jnp.where(high_id == tall(slot & 255, FC), one, none))
            parts = []
            for t in range(3):
                word = block[(j * 3 + t) * 8 : (j * 3 + t + 1) * 8, :]
                parts.append(((word << 16) >> 16).astype(F32) * scales[t])
                parts.append((word >> 16).astype(F32) * scales[t])
            values = jnp.concatenate(parts, axis=0).astype(BF16)
            low = tall(low, 48)
            splits.append(
                jnp.concatenate([jnp.where(low == BF16(q), values, none) for q in range(4)], axis=0)
            )
        acc[...] += lax.dot_general(
            jnp.concatenate(splits, axis=1), jnp.concatenate(hots, axis=1),
            (((1,), (1,)), ((), ())), preferred_element_type=F32,
        )

    def stage(b, last):
        last = lax.fori_loop(b * 4, b * 4 + 4, fill, last)

        @pl.when(b == 0)
        def _():
            rbuf[0, 0:ROWS, :] = sbuf[0]

        @pl.when(b >= 2)
        def _():
            add_batch(b - 2)

        return last

    last = lax.fori_loop(0, BATCHES, stage, (trial, geno))
    copy_of(DEVICES - 1, last).start()

    def tail(b, carry):
        add_batch(b)
        return carry

    lax.fori_loop(BATCHES - 2, BATCHES, tail, 0)
    for q in range(4):
        out_ref[:, q * FC : (q + 1) * FC] = acc[q * 48 : (q + 1) * 48, :]


def body(probe_signs, trial_rows, trial_cols, ar_rho, res_var, plot_owner, plot_slot):
    smem = pl.BlockSpec(memory_space=pltpu.SMEM)
    vmem = pl.BlockSpec(memory_space=pltpu.VMEM)
    hbm = pl.BlockSpec(memory_space=pl.ANY)
    out = pl.pallas_call(
        kernel,
        out_shape=pltpu.VMEM((3 * PROBES, G_DEV), F32),
        in_specs=[hbm, smem, smem, smem, smem, hbm, hbm],
        out_specs=vmem,
        scratch_shapes=[
            pltpu.SMEM((DEVICES,), I32),
            pltpu.SMEM((DEVICES,), I32),
            pltpu.VMEM((FR, 1, FC), I32),
            pltpu.VMEM((FR, 1, FC), I32),
            pltpu.VMEM((FR, PROBES, FC), I32),
            pltpu.VMEM((FR + 2, PROBES, FC), F32),
            pltpu.VMEM((FR + 2, PROBES, FC), F32),
            pltpu.VMEM((2, PROBES, FC), I32),
            pltpu.VMEM(((FR + 1) * FC, 128), I32),
            pltpu.VMEM((SLOTS, DEVICES), I32),
            pltpu.SMEM((SLOTS, DEVICES), I32),
            pltpu.VMEM((DEVICES, ROWS, 128), I32),
            pltpu.VMEM((DEVICES, PAD_ROWS, 128), I32),
            pltpu.VMEM((SLOTS, 2 * DEVICES), F32),
            pltpu.VMEM((12 * PROBES, FC), F32),
            pltpu.SemaphoreType.DMA((PROBES + 2,)),
            pltpu.SemaphoreType.DMA,
            pltpu.SemaphoreType.DMA((2,)),
            pltpu.SemaphoreType.DMA((2,)),
            pltpu.SemaphoreType.DMA((DEVICES,)),
            pltpu.SemaphoreType.DMA((DEVICES,)),
        ],
        compiler_params=pltpu.CompilerParams(
            collective_id=0, has_side_effects=True, vmem_limit_bytes=56 << 20
        ),
        name="hutchinson_exchange",
    )(
        probe_signs.transpose(0, 1, 3, 2, 4).reshape(PROBES, FR, 1, FC),
        trial_rows,
        trial_cols,
        ar_rho,
        res_var,
        plot_owner.transpose(0, 1, 2, 4, 3).reshape(FR, 1, FC),
        plot_slot.transpose(0, 2, 1, 3).reshape(FR, 1, FC),
    )
    return out.reshape(3, PROBES, G_DEV)


def solution(mesh):
    return jax.shard_map(
        body,
        mesh=mesh,
        in_specs=(
            P(None, ("trial", "geno"), None, None, None),
            P("trial"),
            P("trial"),
            P("trial", None),
            P("trial"),
            P(("trial", "geno"), None, None, None, None),
            P(("trial", "geno"), None, None, None),
        ),
        out_specs=P(None, None, ("trial", "geno")),
        check_vma=False,
    )
```

```python
import jax
import jax.numpy as jnp
from jax import lax
from jax.experimental import pallas as pl
from jax.experimental.pallas import tpu as pltpu
from jax.sharding import PartitionSpec as P

G_DEV = 1024
PROBES = 16
FR = 44
FC = 256
DEVICES = 128
PER_ROW = 5
WORDS = 24
SLOTS = 176
ROWS = 36
PAD_ROWS = 40
BATCH = 16
BATCHES = DEVICES // BATCH
RANK_ROWS = 22
TERM_ROWS = 7
SCALE_BITS = 24
MESH = pl.DeviceIdType.MESH
F32 = jnp.float32
BF16 = jnp.bfloat16
I32 = jnp.int32


def send_order():
    out = []
    for s in range(1, DEVICES):
        i, near, far = s % 4, s // 4 % 4, s // 16
        out.append((i, near, (far + 2 * near + i) % 4, (far // 4 + near + i // 2) % 2))
    return out


def kernel(
    signs_ref, rows_ref, cols_ref, rho_ref, var_ref, owner_ref, slot_ref, out_ref,
    trials, genos, owners, slots, xs, us, vs, halo, table, picks, picks_s, sbuf, rbuf, digits, acc,
    in_sem, pick_sem, halo_send, halo_recv, send_sem, recv_sem,
):
    trial, geno = lax.axis_index("trial"), lax.axis_index("geno")
    barrier = pltpu.get_barrier_semaphore()

    loads = [
        pltpu.make_async_copy(signs_ref.at[p, :, 0], xs.at[:, p, :], in_sem.at[p])
        for p in range(PROBES)
    ]
    owner_load = pltpu.make_async_copy(owner_ref, owners, in_sem.at[PROBES])
    slot_load = pltpu.make_async_copy(slot_ref, slots, in_sem.at[PROBES + 1])
    for load in [owner_load, *loads, slot_load]:
        load.start()

    z, y, core = trial // 8, lax.rem(trial // 2, 4), lax.rem(trial, 2)
    xs_at = [lax.rem(geno + i, 4) for i in range(4)]
    ys_at = [lax.rem(y + i, 4) * 2 for i in range(4)]
    zs_at = [lax.rem(z + i, 4) * 8 for i in range(4)]
    cores_at = [core, 1 - core]
    trials[0] = trial
    genos[0] = geno
    for s, (dx, dy, dz, dc) in enumerate(send_order(), 1):
        t, g = zs_at[dz] + ys_at[dy] + cores_at[dc], xs_at[dx]
        pl.semaphore_signal(barrier, inc=1, device_id=(t, g), device_id_type=MESH)
        trials[s] = t
        genos[s] = g

    def tall(row, height):
        row = jnp.broadcast_to(row, (16, row.shape[1])).astype(F32).astype(BF16)
        return jnp.concatenate([row] * (height // 16), axis=0)

    def ids(height, width):
        return lax.broadcasted_iota(I32, (height, width), 0).astype(F32).astype(BF16)

    one, none = BF16(1), BF16(0)
    owner_id = ids(DEVICES, FC)
    place_id = ids(SLOTS, FC)
    col_i = lax.broadcasted_iota(I32, (FC, FC), 0)
    col_j = lax.broadcasted_iota(I32, (FC, FC), 1)
    upto = jnp.where(col_i <= col_j, F32(1), F32(0)).astype(BF16)
    col_no = tall(lax.broadcasted_iota(I32, (1, FC), 1), DEVICES)
    digits[...] = jnp.zeros_like(digits)
    owner_load.wait()

    def rank_rows(q, running):
        owns = [owner_id == tall(owners[q * RANK_ROWS + i], DEVICES) for i in range(RANK_ROWS)]
        hots = jnp.concatenate([jnp.where(own, one, none) for own in owns], axis=0)
        counts = jnp.dot(hots, upto, preferred_element_type=F32)
        lefts, rights = [], []
        for i, own in enumerate(owns):
            count = counts[i * DEVICES : (i + 1) * DEVICES]
            before = jnp.concatenate([running.astype(BF16)] * 2, axis=1)
            running = running + jnp.broadcast_to(count[:, FC - 1 :], (DEVICES, 128))
            mine = jnp.where(own, count.astype(BF16) + before, none)
            parts = [mine[j * 16 : (j + 1) * 16] for j in range(DEVICES // 16)]
            while len(parts) > 1:
                parts = [x + y for x, y in zip(parts[::2], parts[1::2])]
            place = jnp.sum(parts[0].astype(F32), axis=0, keepdims=True) - 1.0
            lefts.append(jnp.where(place_id == tall(place, SLOTS), one, none))
            row_no = tall(jnp.full((1, FC), q * RANK_ROWS + i + 1, I32), DEVICES)
            rights.append(
                jnp.concatenate([jnp.where(own, row_no, none), jnp.where(own, col_no, none)], axis=0)
            )
        digits[...] += lax.dot_general(
            jnp.concatenate(lefts, axis=1), jnp.concatenate(rights, axis=1),
            (((1,), (1,)), ((), ())), preferred_element_type=F32,
        )
        return running

    lax.fori_loop(0, FR // RANK_ROWS, rank_rows, jnp.zeros((DEVICES, 128), F32))
    plot = (digits[:, :DEVICES] * float(FC) + digits[:, DEVICES:]).astype(I32)
    picks[...] = jnp.clip(plot, 0, (FR + 1) * FC - 1)
    to_smem = pltpu.make_async_copy(picks, picks_s, pick_sem)
    to_smem.start()

    n_rows, n_cols = rows_ref[0], cols_ref[0]
    rho_r = jnp.full((1, FC), rho_ref[0, 0], F32)
    rho_c = jnp.full((1, FC), rho_ref[0, 1], F32)
    res = jnp.full((1, FC), var_ref[0], F32)
    col = lax.broadcasted_iota(I32, (1, FC), 1)

    def line(rho):
        inv = 1.0 / (1.0 - rho * rho)
        inside = 1.0 + rho * rho
        return (
            (inv, inv * inside, -inv * rho),
            (2.0 * rho * inv * inv, 4.0 * rho * inv * inv, -inside * inv * inv),
        )

    (ce, ci, co), (cse, csi, cso) = line(rho_c)
    (re, ri, ro), (rse, rsi, rso) = line(rho_r)
    col_edge = (col == 0) | (col == n_cols - 1)
    cd = jnp.where(col_edge, ce, ci)
    csd = jnp.where(col_edge, cse, csi)
    in_col = col < n_cols
    left_ok = col > 0
    right_ok = col < FC - 1
    inv_res = 1.0 / res
    c_top = jnp.maximum(ce, ci) - 2.0 * co
    cs_top = jnp.maximum(cse, csi) - 2.0 * cso
    r_top = jnp.maximum(re, ri) - 2.0 * ro
    rs_top = jnp.maximum(rse, rsi) - 2.0 * rso
    tops = [r_top * c_top * inv_res, rs_top * c_top * inv_res, r_top * cs_top * inv_res]
    scale_ints = [jnp.ceil(top * float(1 << SCALE_BITS)).astype(I32) + 1 for top in tops]
    gains = [
        inv_res * 32766.0 / (s.astype(F32) * (1.0 / float(1 << SCALE_BITS))) for s in scale_ints
    ]
    sub8 = lax.broadcasted_iota(I32, (8, FC), 0)
    scale_rows = jnp.where(
        sub8 == 5, scale_ints[0], jnp.where(sub8 == 6, scale_ints[1], scale_ints[2])
    )

    lane = lax.broadcasted_iota(I32, (1, 128), 1)
    group = jnp.where(lane < PER_ROW * WORDS, lane // WORDS, lane - PER_ROW * WORDS)
    group = jnp.where(group >= PER_ROW, 0, group)
    masks = [group == j for j in range(PER_ROW)]
    lane8 = lax.broadcasted_iota(I32, (8, 128), 1)
    first_scales = jnp.where(
        lane8 == 125, scale_ints[0][:, :128],
        jnp.where(lane8 == 126, scale_ints[1][:, :128], scale_ints[2][:, :128]),
    )
    table[0:8, :] = jnp.where(lane8 >= 125, first_scales, jnp.where(lane8 >= 120, -1, 0))

    for load in [*loads, slot_load]:
        load.wait()

    def columns(bits, row):
        present = in_col & (row >= 0) & (row < n_rows)
        p = jnp.where(present, 2.0 * bits.astype(F32) - 1.0, F32(0))
        beside = jnp.where(left_ok, pltpu.roll(p, 1, 1), F32(0)) + jnp.where(
            right_ok, pltpu.roll(p, FC - 1, 1), F32(0)
        )
        return cd * p + co * beside, csd * p + cso * beside

    def columns_rows(q, carry):
        for i in range(4):
            r = q * 4 + i
            u, v = columns(xs[r], geno * FR + r)
            us[r + 1] = u
            vs[r + 1] = v
        return carry

    lax.fori_loop(0, FR // 4, columns_rows, 0)

    pl.semaphore_wait(barrier, DEVICES - 1)
    above = (trial, lax.rem(geno + 3, 4))
    below = (trial, lax.rem(geno + 1, 4))
    edges = [
        pltpu.make_async_remote_copy(
            src_ref=xs.at[0], dst_ref=halo.at[1], send_sem=halo_send.at[0],
            recv_sem=halo_recv.at[1], device_id=above, device_id_type=MESH,
        ),
        pltpu.make_async_remote_copy(
            src_ref=xs.at[FR - 1], dst_ref=halo.at[0], send_sem=halo_send.at[1],
            recv_sem=halo_recv.at[0], device_id=below, device_id_type=MESH,
        ),
    ]
    for edge in edges:
        edge.start()

    def terms_row(r):
        row = geno * FR + r
        edge = (row == 0) | (row == n_rows - 1)
        rd = jnp.where(edge, re, ri)
        rsd = jnp.where(edge, rse, rsi)
        present = in_col & (row < n_rows)
        k0, k1, k2 = [jnp.where(present, gain, F32(0)) for gain in gains]
        u, v = us[r + 1], vs[r + 1]
        u2 = us[r] + us[r + 2]
        v2 = vs[r] + vs[r + 2]
        values = [
            (rd * u + ro * u2) * k0,
            (rsd * u + rso * u2) * k1,
            (rd * v + ro * v2) * k2,
        ]
        words = []
        for value in values:
            q = jnp.floor(value + 0.5).astype(I32)
            words.append((q[8:] << 16) | (q[:8] & 0xFFFF))
        aux = jnp.where(sub8 < PER_ROW, slots[r], scale_rows)
        stacked = jnp.concatenate(words * PER_ROW + [aux], axis=0)
        table[pl.ds(pl.multiple_of((r + 1) * FC, FC), FC), :] = stacked.T

    def inner_rows(q, carry):
        for i in range(TERM_ROWS):
            terms_row(1 + q * TERM_ROWS + i)
        return carry

    lax.fori_loop(0, (FR - 2) // TERM_ROWS, inner_rows, 0)
    for edge in edges:
        edge.wait()
    for side, r in ((0, -1), (1, FR)):
        row = jnp.where((geno == 0) & (side == 0), -1, geno * FR + r)
        u, v = columns(halo[side], row)
        us[r + 1] = u
        vs[r + 1] = v

    def outer_row(i, carry):
        terms_row(i * (FR - 1))
        return carry

    lax.fori_loop(0, 2, outer_row, 0)
    to_smem.wait()

    def gather(target, dst):
        for r in range(ROWS):
            row = None
            for j in range(PER_ROW):
                place = min(r * PER_ROW + j, SLOTS - 1)
                part = table[pl.ds(picks_s.at[place][target], 1), :]
                if r * PER_ROW + j >= SLOTS:
                    part = table[0:1, :]
                row = part if row is None else jnp.where(masks[j], part, row)
            dst[pl.ds(r, 1), :] = row

    def copy_of(s, target=None):
        return pltpu.make_async_remote_copy(
            src_ref=sbuf.at[s], dst_ref=rbuf.at[s, pl.ds(0, ROWS)],
            send_sem=send_sem.at[s], recv_sem=recv_sem.at[s],
            device_id=below if target is None else target, device_id_type=MESH,
        )

    acc[...] = jnp.zeros_like(acc)

    def fill(step, last):
        for i in range(4):
            s = step * 4 + i
            target = trials[s], genos[s]
            gather(target[0] * 4 + target[1], sbuf.at[s])
            if i < 2:

                @pl.when(step > 0)
                def _(s=s, last=last):
                    copy_of(s - 1, last).start()

            else:
                copy_of(s - 1, last).start()
            last = target
        return last

    width = BATCH * PAD_ROWS
    high_id = ids(FC, width)
    pos = lax.rem(lax.broadcasted_iota(I32, (1, width), 1), PAD_ROWS)

    def add_batch(b):
        def arrive(s, carry):
            copy_of(s).wait()
            return carry

        lax.fori_loop(jnp.maximum(b * BATCH, 1), (b + 1) * BATCH, arrive, 0)
        block = rbuf[pl.ds(b * BATCH, BATCH)].reshape(width, 128).T
        scales = [
            block[125 + t : 126 + t, :].astype(F32) * (1.0 / (float(1 << SCALE_BITS) * 32766.0))
            for t in range(3)
        ]
        splits, hots = [], []
        for j in range(PER_ROW):
            slot = jnp.where(pos < ROWS, block[120 + j : 121 + j, :], -1)
            low = slot >> 8
            hots.append(jnp.where(high_id == tall(slot & 255, FC), one, none))
            parts = []
            for t in range(3):
                word = block[(j * 3 + t) * 8 : (j * 3 + t + 1) * 8, :]
                parts.append(((word << 16) >> 16).astype(F32) * scales[t])
                parts.append((word >> 16).astype(F32) * scales[t])
            values = jnp.concatenate(parts, axis=0).astype(BF16)
            low = tall(low, 48)
            splits.append(
                jnp.concatenate([jnp.where(low == BF16(q), values, none) for q in range(4)], axis=0)
            )
        acc[...] += lax.dot_general(
            jnp.concatenate(splits, axis=1), jnp.concatenate(hots, axis=1),
            (((1,), (1,)), ((), ())), preferred_element_type=F32,
        )

    def stage(b, last):
        last = lax.fori_loop(b * 4, b * 4 + 4, fill, last)

        @pl.when(b == 0)
        def _():
            rbuf[0, 0:ROWS, :] = sbuf[0]

        @pl.when(b >= 2)
        def _():
            add_batch(b - 2)

        return last

    last = lax.fori_loop(0, BATCHES, stage, (trial, geno))
    copy_of(DEVICES - 1, last).start()

    def tail(b, carry):
        add_batch(b)
        return carry

    lax.fori_loop(BATCHES - 2, BATCHES, tail, 0)
    for q in range(4):
        out_ref[:, q * FC : (q + 1) * FC] = acc[q * 48 : (q + 1) * 48, :]


def body(probe_signs, trial_rows, trial_cols, ar_rho, res_var, plot_owner, plot_slot):
    smem = pl.BlockSpec(memory_space=pltpu.SMEM)
    vmem = pl.BlockSpec(memory_space=pltpu.VMEM)
    hbm = pl.BlockSpec(memory_space=pl.ANY)
    out = pl.pallas_call(
        kernel,
        out_shape=pltpu.VMEM((3 * PROBES, G_DEV), F32),
        in_specs=[hbm, smem, smem, smem, smem, hbm, hbm],
        out_specs=vmem,
        scratch_shapes=[
            pltpu.SMEM((DEVICES,), I32),
            pltpu.SMEM((DEVICES,), I32),
            pltpu.VMEM((FR, 1, FC), I32),
            pltpu.VMEM((FR, 1, FC), I32),
            pltpu.VMEM((FR, PROBES, FC), I32),
            pltpu.VMEM((FR + 2, PROBES, FC), F32),
            pltpu.VMEM((FR + 2, PROBES, FC), F32),
            pltpu.VMEM((2, PROBES, FC), I32),
            pltpu.VMEM(((FR + 1) * FC, 128), I32),
            pltpu.VMEM((SLOTS, DEVICES), I32),
            pltpu.SMEM((SLOTS, DEVICES), I32),
            pltpu.VMEM((DEVICES, ROWS, 128), I32),
            pltpu.VMEM((DEVICES, PAD_ROWS, 128), I32),
            pltpu.VMEM((SLOTS, 2 * DEVICES), F32),
            pltpu.VMEM((12 * PROBES, FC), F32),
            pltpu.SemaphoreType.DMA((PROBES + 2,)),
            pltpu.SemaphoreType.DMA,
            pltpu.SemaphoreType.DMA((2,)),
            pltpu.SemaphoreType.DMA((2,)),
            pltpu.SemaphoreType.DMA((DEVICES,)),
            pltpu.SemaphoreType.DMA((DEVICES,)),
        ],
        compiler_params=pltpu.CompilerParams(
            collective_id=0, has_side_effects=True, vmem_limit_bytes=56 << 20
        ),
        name="hutchinson_exchange",
    )(
        probe_signs.transpose(0, 1, 3, 2, 4).reshape(PROBES, FR, 1, FC),
        trial_rows,
        trial_cols,
        ar_rho,
        res_var,
        plot_owner.transpose(0, 1, 2, 4, 3).reshape(FR, 1, FC),
        plot_slot.transpose(0, 2, 1, 3).reshape(FR, 1, FC),
    )
    return out.reshape(3, PROBES, G_DEV)


def solution(mesh):
    return jax.shard_map(
        body,
        mesh=mesh,
        in_specs=(
            P(None, ("trial", "geno"), None, None, None),
            P("trial"),
            P("trial"),
            P("trial", None),
            P("trial"),
            P(("trial", "geno"), None, None, None, None),
            P(("trial", "geno"), None, None, None),
        ),
        out_specs=P(None, None, ("trial", "geno")),
        check_vma=False,
    )
```

```python
import jax
import jax.numpy as jnp
from jax import lax
from jax.experimental import pallas as pl
from jax.experimental.pallas import tpu as pltpu
from jax.sharding import PartitionSpec as P

G_DEV = 1024
PROBES = 16
FR = 44
FC = 256
DEVICES = 128
PER_ROW = 5
WORDS = 24
SLOTS = 176
ROWS = 36
PAD_ROWS = 40
BATCH = 16
BATCHES = DEVICES // BATCH
RANK_ROWS = 22
TERM_ROWS = 7
SCALE_BITS = 24
MESH = pl.DeviceIdType.MESH
F32 = jnp.float32
BF16 = jnp.bfloat16
I32 = jnp.int32


def send_order():
    out = []
    for s in range(1, DEVICES):
        i, near, far = s % 4, s // 4 % 4, s // 16
        out.append((near, i, (far + 2 * near + i) % 4, (far // 4 + near + i // 2) % 2))
    return out


def kernel(
    signs_ref, rows_ref, cols_ref, rho_ref, var_ref, owner_ref, slot_ref, out_ref,
    trials, genos, owners, slots, xs, us, vs, halo, table, picks, picks_s, sbuf, rbuf, digits, acc,
    in_sem, pick_sem, halo_send, halo_recv, send_sem, recv_sem,
):
    trial, geno = lax.axis_index("trial"), lax.axis_index("geno")
    barrier = pltpu.get_barrier_semaphore()

    loads = [
        pltpu.make_async_copy(signs_ref.at[p, :, 0], xs.at[:, p, :], in_sem.at[p])
        for p in range(PROBES)
    ]
    owner_load = pltpu.make_async_copy(owner_ref, owners, in_sem.at[PROBES])
    slot_load = pltpu.make_async_copy(slot_ref, slots, in_sem.at[PROBES + 1])
    for load in [owner_load, *loads, slot_load]:
        load.start()

    z, y, core = trial // 8, lax.rem(trial // 2, 4), lax.rem(trial, 2)
    xs_at = [lax.rem(geno + i, 4) for i in range(4)]
    ys_at = [lax.rem(y + i, 4) * 2 for i in range(4)]
    zs_at = [lax.rem(z + i, 4) * 8 for i in range(4)]
    cores_at = [core, 1 - core]
    trials[0] = trial
    genos[0] = geno
    for s, (dx, dy, dz, dc) in enumerate(send_order(), 1):
        t, g = zs_at[dz] + ys_at[dy] + cores_at[dc], xs_at[dx]
        pl.semaphore_signal(barrier, inc=1, device_id=(t, g), device_id_type=MESH)
        trials[s] = t
        genos[s] = g

    def tall(row, height):
        row = jnp.broadcast_to(row, (16, row.shape[1])).astype(F32).astype(BF16)
        return jnp.concatenate([row] * (height // 16), axis=0)

    def ids(height, width):
        return lax.broadcasted_iota(I32, (height, width), 0).astype(F32).astype(BF16)

    one, none = BF16(1), BF16(0)
    owner_id = ids(DEVICES, FC)
    place_id = ids(SLOTS, FC)
    col_i = lax.broadcasted_iota(I32, (FC, FC), 0)
    col_j = lax.broadcasted_iota(I32, (FC, FC), 1)
    upto = jnp.where(col_i <= col_j, F32(1), F32(0)).astype(BF16)
    col_no = tall(lax.broadcasted_iota(I32, (1, FC), 1), DEVICES)
    digits[...] = jnp.zeros_like(digits)
    owner_load.wait()

    def rank_rows(q, running):
        owns = [owner_id == tall(owners[q * RANK_ROWS + i], DEVICES) for i in range(RANK_ROWS)]
        hots = jnp.concatenate([jnp.where(own, one, none) for own in owns], axis=0)
        counts = jnp.dot(hots, upto, preferred_element_type=F32)
        lefts, rights = [], []
        for i, own in enumerate(owns):
            count = counts[i * DEVICES : (i + 1) * DEVICES]
            before = jnp.concatenate([running.astype(BF16)] * 2, axis=1)
            running = running + jnp.broadcast_to(count[:, FC - 1 :], (DEVICES, 128))
            mine = jnp.where(own, count.astype(BF16) + before, none)
            parts = [mine[j * 16 : (j + 1) * 16] for j in range(DEVICES // 16)]
            while len(parts) > 1:
                parts = [x + y for x, y in zip(parts[::2], parts[1::2])]
            place = jnp.sum(parts[0].astype(F32), axis=0, keepdims=True) - 1.0
            lefts.append(jnp.where(place_id == tall(place, SLOTS), one, none))
            row_no = tall(jnp.full((1, FC), q * RANK_ROWS + i + 1, I32), DEVICES)
            rights.append(
                jnp.concatenate([jnp.where(own, row_no, none), jnp.where(own, col_no, none)], axis=0)
            )
        digits[...] += lax.dot_general(
            jnp.concatenate(lefts, axis=1), jnp.concatenate(rights, axis=1),
            (((1,), (1,)), ((), ())), preferred_element_type=F32,
        )
        return running

    lax.fori_loop(0, FR // RANK_ROWS, rank_rows, jnp.zeros((DEVICES, 128), F32))
    plot = (digits[:, :DEVICES] * float(FC) + digits[:, DEVICES:]).astype(I32)
    picks[...] = jnp.clip(plot, 0, (FR + 1) * FC - 1)
    to_smem = pltpu.make_async_copy(picks, picks_s, pick_sem)
    to_smem.start()

    n_rows, n_cols = rows_ref[0], cols_ref[0]
    rho_r = jnp.full((1, FC), rho_ref[0, 0], F32)
    rho_c = jnp.full((1, FC), rho_ref[0, 1], F32)
    res = jnp.full((1, FC), var_ref[0], F32)
    col = lax.broadcasted_iota(I32, (1, FC), 1)

    def line(rho):
        inv = 1.0 / (1.0 - rho * rho)
        inside = 1.0 + rho * rho
        return (
            (inv, inv * inside, -inv * rho),
            (2.0 * rho * inv * inv, 4.0 * rho * inv * inv, -inside * inv * inv),
        )

    (ce, ci, co), (cse, csi, cso) = line(rho_c)
    (re, ri, ro), (rse, rsi, rso) = line(rho_r)
    col_edge = (col == 0) | (col == n_cols - 1)
    cd = jnp.where(col_edge, ce, ci)
    csd = jnp.where(col_edge, cse, csi)
    in_col = col < n_cols
    left_ok = col > 0
    right_ok = col < FC - 1
    inv_res = 1.0 / res
    c_top = jnp.maximum(ce, ci) - 2.0 * co
    cs_top = jnp.maximum(cse, csi) - 2.0 * cso
    r_top = jnp.maximum(re, ri) - 2.0 * ro
    rs_top = jnp.maximum(rse, rsi) - 2.0 * rso
    tops = [r_top * c_top * inv_res, rs_top * c_top * inv_res, r_top * cs_top * inv_res]
    scale_ints = [jnp.ceil(top * float(1 << SCALE_BITS)).astype(I32) + 1 for top in tops]
    gains = [
        inv_res * 32766.0 / (s.astype(F32) * (1.0 / float(1 << SCALE_BITS))) for s in scale_ints
    ]
    sub8 = lax.broadcasted_iota(I32, (8, FC), 0)
    scale_rows = jnp.where(
        sub8 == 5, scale_ints[0], jnp.where(sub8 == 6, scale_ints[1], scale_ints[2])
    )

    lane = lax.broadcasted_iota(I32, (1, 128), 1)
    group = jnp.where(lane < PER_ROW * WORDS, lane // WORDS, lane - PER_ROW * WORDS)
    group = jnp.where(group >= PER_ROW, 0, group)
    masks = [group == j for j in range(PER_ROW)]
    lane8 = lax.broadcasted_iota(I32, (8, 128), 1)
    first_scales = jnp.where(
        lane8 == 125, scale_ints[0][:, :128],
        jnp.where(lane8 == 126, scale_ints[1][:, :128], scale_ints[2][:, :128]),
    )
    table[0:8, :] = jnp.where(lane8 >= 125, first_scales, jnp.where(lane8 >= 120, -1, 0))

    for load in [*loads, slot_load]:
        load.wait()

    def columns(bits, row):
        present = in_col & (row >= 0) & (row < n_rows)
        p = jnp.where(present, 2.0 * bits.astype(F32) - 1.0, F32(0))
        beside = jnp.where(left_ok, pltpu.roll(p, 1, 1), F32(0)) + jnp.where(
            right_ok, pltpu.roll(p, FC - 1, 1), F32(0)
        )
        return cd * p + co * beside, csd * p + cso * beside

    def columns_rows(q, carry):
        for i in range(4):
            r = q * 4 + i
            u, v = columns(xs[r], geno * FR + r)
            us[r + 1] = u
            vs[r + 1] = v
        return carry

    lax.fori_loop(0, FR // 4, columns_rows, 0)

    pl.semaphore_wait(barrier, DEVICES - 1)
    above = (trial, lax.rem(geno + 3, 4))
    below = (trial, lax.rem(geno + 1, 4))
    edges = [
        pltpu.make_async_remote_copy(
            src_ref=xs.at[0], dst_ref=halo.at[1], send_sem=halo_send.at[0],
            recv_sem=halo_recv.at[1], device_id=above, device_id_type=MESH,
        ),
        pltpu.make_async_remote_copy(
            src_ref=xs.at[FR - 1], dst_ref=halo.at[0], send_sem=halo_send.at[1],
            recv_sem=halo_recv.at[0], device_id=below, device_id_type=MESH,
        ),
    ]
    for edge in edges:
        edge.start()

    def terms_row(r):
        row = geno * FR + r
        edge = (row == 0) | (row == n_rows - 1)
        rd = jnp.where(edge, re, ri)
        rsd = jnp.where(edge, rse, rsi)
        present = in_col & (row < n_rows)
        k0, k1, k2 = [jnp.where(present, gain, F32(0)) for gain in gains]
        u, v = us[r + 1], vs[r + 1]
        u2 = us[r] + us[r + 2]
        v2 = vs[r] + vs[r + 2]
        values = [
            (rd * u + ro * u2) * k0,
            (rsd * u + rso * u2) * k1,
            (rd * v + ro * v2) * k2,
        ]
        words = []
        for value in values:
            q = jnp.floor(value + 0.5).astype(I32)
            words.append((q[8:] << 16) | (q[:8] & 0xFFFF))
        aux = jnp.where(sub8 < PER_ROW, slots[r], scale_rows)
        stacked = jnp.concatenate(words * PER_ROW + [aux], axis=0)
        table[pl.ds(pl.multiple_of((r + 1) * FC, FC), FC), :] = stacked.T

    def inner_rows(q, carry):
        for i in range(TERM_ROWS):
            terms_row(1 + q * TERM_ROWS + i)
        return carry

    lax.fori_loop(0, (FR - 2) // TERM_ROWS, inner_rows, 0)
    for edge in edges:
        edge.wait()
    for side, r in ((0, -1), (1, FR)):
        row = jnp.where((geno == 0) & (side == 0), -1, geno * FR + r)
        u, v = columns(halo[side], row)
        us[r + 1] = u
        vs[r + 1] = v

    def outer_row(i, carry):
        terms_row(i * (FR - 1))
        return carry

    lax.fori_loop(0, 2, outer_row, 0)
    to_smem.wait()

    def gather(target, dst):
        for r in range(ROWS):
            row = None
            for j in range(PER_ROW):
                place = min(r * PER_ROW + j, SLOTS - 1)
                part = table[pl.ds(picks_s.at[place][target], 1), :]
                if r * PER_ROW + j >= SLOTS:
                    part = table[0:1, :]
                row = part if row is None else jnp.where(masks[j], part, row)
            dst[pl.ds(r, 1), :] = row

    def copy_of(s, target=None):
        return pltpu.make_async_remote_copy(
            src_ref=sbuf.at[s], dst_ref=rbuf.at[s, pl.ds(0, ROWS)],
            send_sem=send_sem.at[s], recv_sem=recv_sem.at[s],
            device_id=below if target is None else target, device_id_type=MESH,
        )

    acc[...] = jnp.zeros_like(acc)

    def fill(step, last):
        for i in range(4):
            s = step * 4 + i
            target = trials[s], genos[s]
            gather(target[0] * 4 + target[1], sbuf.at[s])
            if i < 2:

                @pl.when(step > 0)
                def _(s=s, last=last):
                    copy_of(s - 1, last).start()

            else:
                copy_of(s - 1, last).start()
            last = target
        return last

    width = BATCH * PAD_ROWS
    high_id = ids(FC, width)
    pos = lax.rem(lax.broadcasted_iota(I32, (1, width), 1), PAD_ROWS)

    def add_batch(b):
        def arrive(s, carry):
            copy_of(s).wait()
            return carry

        lax.fori_loop(jnp.maximum(b * BATCH, 1), (b + 1) * BATCH, arrive, 0)
        block = rbuf[pl.ds(b * BATCH, BATCH)].reshape(width, 128).T
        scales = [
            block[125 + t : 126 + t, :].astype(F32) * (1.0 / (float(1 << SCALE_BITS) * 32766.0))
            for t in range(3)
        ]
        splits, hots = [], []
        for j in range(PER_ROW):
            slot = jnp.where(pos < ROWS, block[120 + j : 121 + j, :], -1)
            low = slot >> 8
            hots.append(jnp.where(high_id == tall(slot & 255, FC), one, none))
            parts = []
            for t in range(3):
                word = block[(j * 3 + t) * 8 : (j * 3 + t + 1) * 8, :]
                parts.append(((word << 16) >> 16).astype(F32) * scales[t])
                parts.append((word >> 16).astype(F32) * scales[t])
            values = jnp.concatenate(parts, axis=0).astype(BF16)
            low = tall(low, 48)
            splits.append(
                jnp.concatenate([jnp.where(low == BF16(q), values, none) for q in range(4)], axis=0)
            )
        acc[...] += lax.dot_general(
            jnp.concatenate(splits, axis=1), jnp.concatenate(hots, axis=1),
            (((1,), (1,)), ((), ())), preferred_element_type=F32,
        )

    def stage(b, last):
        last = lax.fori_loop(b * 4, b * 4 + 4, fill, last)

        @pl.when(b == 0)
        def _():
            rbuf[0, 0:ROWS, :] = sbuf[0]

        @pl.when(b >= 2)
        def _():
            add_batch(b - 2)

        return last

    last = lax.fori_loop(0, BATCHES, stage, (trial, geno))
    copy_of(DEVICES - 1, last).start()

    def tail(b, carry):
        add_batch(b)
        return carry

    lax.fori_loop(BATCHES - 2, BATCHES, tail, 0)
    for q in range(4):
        out_ref[:, q * FC : (q + 1) * FC] = acc[q * 48 : (q + 1) * 48, :]


def body(probe_signs, trial_rows, trial_cols, ar_rho, res_var, plot_owner, plot_slot):
    smem = pl.BlockSpec(memory_space=pltpu.SMEM)
    vmem = pl.BlockSpec(memory_space=pltpu.VMEM)
    hbm = pl.BlockSpec(memory_space=pl.ANY)
    out = pl.pallas_call(
        kernel,
        out_shape=pltpu.VMEM((3 * PROBES, G_DEV), F32),
        in_specs=[hbm, smem, smem, smem, smem, hbm, hbm],
        out_specs=vmem,
        scratch_shapes=[
            pltpu.SMEM((DEVICES,), I32),
            pltpu.SMEM((DEVICES,), I32),
            pltpu.VMEM((FR, 1, FC), I32),
            pltpu.VMEM((FR, 1, FC), I32),
            pltpu.VMEM((FR, PROBES, FC), I32),
            pltpu.VMEM((FR + 2, PROBES, FC), F32),
            pltpu.VMEM((FR + 2, PROBES, FC), F32),
            pltpu.VMEM((2, PROBES, FC), I32),
            pltpu.VMEM(((FR + 1) * FC, 128), I32),
            pltpu.VMEM((SLOTS, DEVICES), I32),
            pltpu.SMEM((SLOTS, DEVICES), I32),
            pltpu.VMEM((DEVICES, ROWS, 128), I32),
            pltpu.VMEM((DEVICES, PAD_ROWS, 128), I32),
            pltpu.VMEM((SLOTS, 2 * DEVICES), F32),
            pltpu.VMEM((12 * PROBES, FC), F32),
            pltpu.SemaphoreType.DMA((PROBES + 2,)),
            pltpu.SemaphoreType.DMA,
            pltpu.SemaphoreType.DMA((2,)),
            pltpu.SemaphoreType.DMA((2,)),
            pltpu.SemaphoreType.DMA((DEVICES,)),
            pltpu.SemaphoreType.DMA((DEVICES,)),
        ],
        compiler_params=pltpu.CompilerParams(
            collective_id=0, has_side_effects=True, vmem_limit_bytes=56 << 20
        ),
        name="hutchinson_exchange",
    )(
        probe_signs.transpose(0, 1, 3, 2, 4).reshape(PROBES, FR, 1, FC),
        trial_rows,
        trial_cols,
        ar_rho,
        res_var,
        plot_owner.transpose(0, 1, 2, 4, 3).reshape(FR, 1, FC),
        plot_slot.transpose(0, 2, 1, 3).reshape(FR, 1, FC),
    )
    return out.reshape(3, PROBES, G_DEV)


def solution(mesh):
    return jax.shard_map(
        body,
        mesh=mesh,
        in_specs=(
            P(None, ("trial", "geno"), None, None, None),
            P("trial"),
            P("trial"),
            P("trial", None),
            P("trial"),
            P(("trial", "geno"), None, None, None, None),
            P(("trial", "geno"), None, None, None),
        ),
        out_specs=P(None, None, ("trial", "geno")),
        check_vma=False,
    )
```
